32 devices in a mesh: tp: 4 (over z), cp: 8 (over y, x, core).
Axes of the slice: x: 2, y: 2, z: 4, core: 2. Of those that a mesh axis runs over, the one named last changes fastest.
Arguments:
- query: bfloat16 [16, 1024, 64, 128], P(None, 'cp', 'tp'), parts along dimension 2
- keys: bfloat16 [16, 1024, 8, 128], P(None, 'cp', 'tp'), parts along dimension 2
- values: bfloat16 [16, 1024, 8, 128], P(None, 'cp', 'tp'), parts along dimension 2
- positions: int32 [16, 1024], P(None, 'cp')
- grad_out: bfloat16 [16, 1024, 64, 128], P(None, 'cp', 'tp'), parts along dimension 2
Outputs:
- output 1: bfloat16 [16, 1024, 64, 128], P(None, 'cp', 'tp'), parts along dimension 2
- output 2: bfloat16 [16, 1024, 64, 128], P(None, 'cp', 'tp'), parts along dimension 2
- output 3: bfloat16 [16, 1024, 8, 128], P(None, 'cp', 'tp'), parts along dimension 2
- output 4: bfloat16 [16, 1024, 8, 128], P(None, 'cp', 'tp'), parts along dimension 2
There are 4 independent parts. The reference program is written for one: setup_inputs(seed, part) draws one part's arguments, and reference() takes and returns one part's arrays. A program takes and returns all parts, laid end to end along the dimension named above; an argument that names none is the same for every part.
All inputs are finite; a program needn't handle non-finite values.
Results may differ from the reference program's by a relative error of at most 0.00828099.
Values are sent between devices in bfloat16 or wider.
A program may use at most 1 GiB of HBM per device.

```python
import jax
import jax.numpy as jnp
from jax import lax

BATCH = 16
SEQ_LEN = 1024
CP_SIZE = 8
PART_HEADS = 16
PART_KV_HEADS = 2
HEAD_DIM = 128
ROPE_THETA = 1000000
QUERY_BLOCK = 128

GROUP_SIZE = PART_HEADS // PART_KV_HEADS
LOCAL_LEN = SEQ_LEN // CP_SIZE
HALF_LEN = LOCAL_LEN // 2
NUM_BLOCKS = SEQ_LEN // QUERY_BLOCK


def layout_index():
    stored = jnp.arange(SEQ_LEN, dtype=jnp.int32)
    device = stored // LOCAL_LEN
    within = stored % LOCAL_LEN
    piece_id = jnp.where(within < HALF_LEN, device, 2 * CP_SIZE - 1 - device)
    return piece_id * HALF_LEN + within % HALF_LEN


def draw_positions(pos_key):
    offset_key, gap_key = jax.random.split(pos_key)
    offsets = jax.random.randint(offset_key, (BATCH, 1), 0, SEQ_LEN, dtype=jnp.int32)
    gaps = jax.random.randint(gap_key, (BATCH, SEQ_LEN), 1, 3, dtype=jnp.int32)
    seq_pos = offsets + jnp.cumsum(gaps, axis=1) - gaps[:, :1]
    return jnp.take(seq_pos, layout_index(), axis=1)


def setup_inputs(seed: int = 0, part: int = 0) -> dict:
    base_key = jax.random.key(seed)
    shared_key, part_root = jax.random.split(base_key)
    part_key = jax.random.fold_in(part_root, part)
    key_query, key_keys, key_values, key_grad = jax.random.split(part_key, 4)
    q_shape = (BATCH, SEQ_LEN, PART_HEADS, HEAD_DIM)
    kv_shape = (BATCH, SEQ_LEN, PART_KV_HEADS, HEAD_DIM)
    return {
        'query': jax.random.normal(key_query, q_shape, jnp.float32).astype(jnp.bfloat16),
        'keys': jax.random.normal(key_keys, kv_shape, jnp.float32).astype(jnp.bfloat16),
        'values': jax.random.normal(key_values, kv_shape, jnp.float32).astype(jnp.bfloat16),
        'positions': draw_positions(shared_key),
        'grad_out': jax.random.normal(key_grad, q_shape, jnp.float32).astype(jnp.bfloat16),
    }


def rotary(tensor, positions, angle_sign):
    half_dim = HEAD_DIM // 2
    freq_expo = jnp.arange(half_dim, dtype=jnp.float32) * (2.0 / HEAD_DIM)
    inv_freq = 1.0 / (ROPE_THETA ** freq_expo)
    angles = positions.astype(jnp.float32)[:, :, None] * inv_freq
    cosine = jnp.cos(angles)[:, :, None, :]
    sine_val = angle_sign * jnp.sin(angles)[:, :, None, :]
    pairs = tensor.astype(jnp.float32).reshape(tensor.shape[:-1] + (half_dim, 2))
    even_part = pairs[..., 0]
    odd_part = pairs[..., 1]
    new_even = even_part * cosine - odd_part * sine_val
    new_odd = even_part * sine_val + odd_part * cosine
    return jnp.stack([new_even, new_odd], axis=-1).reshape(tensor.shape)


def reference(query, keys, values, positions, grad_out):
    score_scale = HEAD_DIM ** -0.5
    q_rot = rotary(query, positions, 1.0).astype(jnp.bfloat16)
    k_rot = rotary(keys, positions, 1.0).astype(jnp.bfloat16)

    def by_group(tensor):
        grouped = tensor.reshape(BATCH, NUM_BLOCKS, QUERY_BLOCK, PART_KV_HEADS, GROUP_SIZE, HEAD_DIM)
        grouped = grouped.transpose(0, 3, 1, 2, 4, 5)
        return grouped.reshape(BATCH * PART_KV_HEADS, NUM_BLOCKS, QUERY_BLOCK, GROUP_SIZE, HEAD_DIM)

    def by_kv(tensor):
        return tensor.transpose(0, 2, 1, 3).reshape(BATCH * PART_KV_HEADS, SEQ_LEN, HEAD_DIM)

    pos_rows = jnp.repeat(positions, PART_KV_HEADS, axis=0)

    def one_group(operands):
        q_blocks, k_group, v_group, g_blocks, pos_group = operands
        k_wide = k_group.astype(jnp.float32)
        v_wide = v_group.astype(jnp.float32)
        qpos_blocks = pos_group.reshape(NUM_BLOCKS, QUERY_BLOCK)

        def block_step(acc_pair, blk_inputs):
            dk_acc, dv_acc = acc_pair
            q_blk, g_blk, q_pos = blk_inputs
            q_wide = q_blk.astype(jnp.float32)
            g_wide = g_blk.astype(jnp.float32)
            scores = jnp.einsum('qgd,kd->gqk', q_wide, k_wide) * score_scale
            visible = pos_group[None, :] <= q_pos[:, None]
            scores = jnp.where(visible[None], scores, -jnp.inf)
            weights = jax.nn.softmax(scores, axis=-1)
            out_blk = jnp.einsum('gqk,kd->qgd', weights, v_wide)
            grad_weights = jnp.einsum('qgd,kd->gqk', g_wide, v_wide)
            row_delta = jnp.sum(weights * grad_weights, axis=-1, keepdims=True)
            grad_scores = weights * (grad_weights - row_delta) * score_scale
            dq_blk = jnp.einsum('gqk,kd->qgd', grad_scores, k_wide)
            dk_acc = dk_acc + jnp.einsum('gqk,qgd->kd', grad_scores, q_wide)
            dv_acc = dv_acc + jnp.einsum('gqk,qgd->kd', weights, g_wide)
            return (dk_acc, dv_acc), (out_blk, dq_blk)

        zero_kv = jnp.zeros((SEQ_LEN, HEAD_DIM), jnp.float32)
        sums, per_block = lax.scan(block_step, (zero_kv, zero_kv), (q_blocks, g_blocks, qpos_blocks))
        return per_block[0], per_block[1], sums[0], sums[1]

    out_all, dq_all, dk_all, dv_all = lax.map(
        one_group, (by_group(q_rot), by_kv(k_rot), by_kv(values), by_group(grad_out), pos_rows))

    def from_group(tensor):
        grouped = tensor.reshape(BATCH, PART_KV_HEADS, NUM_BLOCKS, QUERY_BLOCK, GROUP_SIZE, HEAD_DIM)
        return grouped.transpose(0, 2, 3, 1, 4, 5).reshape(BATCH, SEQ_LEN, PART_HEADS, HEAD_DIM)

    def from_kv(tensor):
        return tensor.reshape(BATCH, PART_KV_HEADS, SEQ_LEN, HEAD_DIM).transpose(0, 2, 1, 3)

    attn_out = from_group(out_all).astype(jnp.bfloat16)
    grad_query = rotary(from_group(dq_all), positions, -1.0).astype(jnp.bfloat16)
    grad_keys = rotary(from_kv(dk_all), positions, -1.0).astype(jnp.bfloat16)
    grad_values = from_kv(dv_all).astype(jnp.bfloat16)
    return (attn_out, grad_query, grad_keys, grad_values)
```

```python
import functools

import jax
import jax.numpy as jnp
from jax import lax
from jax.experimental import pallas as pl
from jax.experimental.pallas import tpu as pltpu
from jax.sharding import PartitionSpec as P

ROPE_THETA = 1000000.0
N_CHUNKS = 4
LOG2E = 1.4426950408889634


def swap_pairs(x):
    lane = lax.broadcasted_iota(jnp.int32, x.shape, 1)
    return jnp.where(lane % 2 == 0, pltpu.roll(x, 127, 1), pltpu.roll(x, 1, 1))


def dot_nt(a, b):
    return lax.dot_general(a, b, (((1,), (1,)), ((), ())), preferred_element_type=jnp.float32)


def dot_nn(a, b):
    return lax.dot_general(a, b, (((1,), (0,)), ((), ())), preferred_element_type=jnp.float32)


def attend_tile(qr, gr, k_view, v_view, n_keys, q_start, scale):
    rows = qr.shape[0]
    blk = 256
    n_blk = n_keys // blk
    scores = []
    for j in range(n_blk):
        s = dot_nt(qr, k_view[j * blk:(j + 1) * blk, :])
        if j == n_blk - 1:
            q_idx = q_start + lax.broadcasted_iota(jnp.int32, s.shape, 0) // 8
            k_idx = j * blk + lax.broadcasted_iota(jnp.int32, s.shape, 1)
            s = jnp.where(k_idx <= q_idx, s, -jnp.inf)
        scores.append(s)
    top = functools.reduce(jnp.maximum, scores)
    row_max = jnp.max(top, axis=1, keepdims=True)
    expo = [jnp.exp2((s - row_max) * (scale * LOG2E)) for s in scores]
    row_sum = jnp.sum(functools.reduce(jnp.add, expo), axis=1, keepdims=True)
    inv = 1.0 / row_sum
    probs = [e * inv for e in expo]
    p_low = [p.astype(jnp.bfloat16) for p in probs]
    p_all = jnp.concatenate(p_low, axis=1)
    out = dot_nn(p_all, v_view[0:n_keys, :])
    delta = jnp.sum(out * gr.astype(jnp.float32), axis=1, keepdims=True)
    ds = []
    for j in range(n_blk):
        dp = dot_nt(gr, v_view[j * blk:(j + 1) * blk, :])
        ds.append((probs[j] * (dp - delta)).astype(jnp.bfloat16))
    ds_all = jnp.concatenate(ds, axis=1)
    dq = dot_nn(ds_all, k_view[0:n_keys, :]) * scale
    dv_t = dot_nn(gr.T, p_all)
    dk_t = dot_nn(qr.T, ds_all)
    return out, dq, dk_t, dv_t


def attention_kernel(cp_size, q_ref, g_ref, cos_ref, sin_ref, kv_ref, *refs):
    out_ref, dq_ref, dkv_ref, qr_s, gr_s, k_s, v_s, o_s, dq_s, dk_s, dv_s = refs[-11:]
    my_index = lax.axis_index('cp')
    length, n_heads, dim = q_ref.shape[1:]
    half = length // 2
    group = n_heads // 2
    scale = dim ** -0.5
    tile = half * group
    cos_g = jnp.broadcast_to(cos_ref[0][:, None, :], (length, group, dim)).reshape(length * group, dim)
    sin_g = jnp.broadcast_to(sin_ref[0][:, None, :], (length, group, dim)).reshape(length * group, dim)
    for h in range(2):
        qx = q_ref[0].astype(jnp.float32)[:, h * group:(h + 1) * group, :].reshape(length * group, dim)
        qr_s[h] = (qx * cos_g + swap_pairs(qx) * sin_g).astype(jnp.bfloat16)
        gx = g_ref[0].astype(jnp.float32)[:, h * group:(h + 1) * group, :].reshape(length * group, dim)
        gr_s[h] = gx.astype(jnp.bfloat16)
        for s in range(cp_size):
            mirror = 2 * cp_size - 1 - s
            k_s[h, s * half:(s + 1) * half, :] = kv_ref[s, 0, h, 0, 0:half, :]
            k_s[h, mirror * half:(mirror + 1) * half, :] = kv_ref[s, 0, h, 0, half:, :]
            v_s[h, s * half:(s + 1) * half, :] = kv_ref[s, 1, h, 0, 0:half, :]
            v_s[h, mirror * half:(mirror + 1) * half, :] = kv_ref[s, 1, h, 0, half:, :]

    def variant(n_low, n_high):
        def one_head(h, carry):
            k_view, v_view = k_s.at[h], v_s.at[h]
            out, dq, dk_t, dv_t = attend_tile(qr_s[h, tile:, :], gr_s[h, tile:, :], k_view, v_view, n_high,
                                              (2 * cp_size - 1 - my_index) * half, scale)
            o_s[h, tile:, :] = out
            dq_s[h, tile:, :] = dq
            dk_s[:, 0:n_high] = dk_t
            dv_s[:, 0:n_high] = dv_t
            if n_high < dk_s.shape[1]:
                dk_s[:, n_high:] = jnp.zeros((dim, dk_s.shape[1] - n_high), jnp.float32)
                dv_s[:, n_high:] = jnp.zeros((dim, dk_s.shape[1] - n_high), jnp.float32)
            out, dq, dk_t, dv_t = attend_tile(qr_s[h, :tile, :], gr_s[h, :tile, :], k_view, v_view, n_low,
                                              my_index * half, scale)
            o_s[h, :tile, :] = out
            dq_s[h, :tile, :] = dq
            dk_s[:, 0:n_low] += dk_t
            dv_s[:, 0:n_low] += dv_t
            for pair in range(cp_size):
                dk_p = dk_s[:, pair * 2 * half:(pair + 1) * 2 * half].T * scale
                dv_p = dv_s[:, pair * 2 * half:(pair + 1) * 2 * half].T
                for sub in range(2):
                    piece = pair * 2 + sub
                    owner, place = (piece, 0) if piece < cp_size else (2 * cp_size - 1 - piece, half)
                    dkv_ref[owner, 0, h, 0, place:place + half, :] = dk_p[sub * half:(sub + 1) * half]
                    dkv_ref[owner, 1, h, 0, place:place + half, :] = dv_p[sub * half:(sub + 1) * half]
            return carry

        lax.fori_loop(0, 2, one_head, 0)

    quarter = cp_size * half // 2

    @pl.when(my_index < cp_size // 2)
    def _():
        variant(quarter, 4 * quarter)

    @pl.when(my_index >= cp_size // 2)
    def _():
        variant(2 * quarter, 3 * quarter)

    outs, grads = [], []
    for h in range(2):
        outs.append(o_s[h].reshape(length, group, dim))
        dqx = dq_s[h]
        grads.append((dqx * cos_g - swap_pairs(dqx) * sin_g).reshape(length, group, dim))
    out_ref[0] = jnp.concatenate(outs, axis=1).astype(jnp.bfloat16)
    dq_ref[0] = jnp.concatenate(grads, axis=1).astype(jnp.bfloat16)


def attention_chunk(query, grad_out, cos_t, sin_t, kv_all, buffers, first, cp_size):
    batch, length, n_heads, dim = query.shape
    n_batch = kv_all.shape[3]
    seq = cp_size * length
    tok_rows = length * (n_heads // 2)
    q_spec = pl.BlockSpec((1, length, n_heads, dim), lambda b: (b + first, 0, 0, 0))
    t_spec = pl.BlockSpec((1, length, dim), lambda b: (b + first, 0, 0))
    kv_spec = pl.BlockSpec((cp_size, 2, 2, 1, length, dim), lambda b: (0, 0, 0, b, 0, 0))
    any_spec = pl.BlockSpec(memory_space=pl.ANY)
    pairs = n_batch * n_heads * length * seq * 5 // 8
    return pl.pallas_call(
        functools.partial(attention_kernel, cp_size),
        grid=(n_batch,),
        out_shape=(jax.ShapeDtypeStruct(query.shape, jnp.bfloat16),
                   jax.ShapeDtypeStruct(query.shape, jnp.bfloat16),
                   jax.ShapeDtypeStruct((cp_size, 2, 2, n_batch, length, dim), jnp.float32)),
        in_specs=[q_spec, q_spec, t_spec, t_spec, kv_spec] + [any_spec] * len(buffers),
        out_specs=(q_spec, q_spec, kv_spec),
        scratch_shapes=[
            pltpu.VMEM((2, tok_rows, dim), jnp.bfloat16),
            pltpu.VMEM((2, tok_rows, dim), jnp.bfloat16),
            pltpu.VMEM((2, seq, dim), jnp.bfloat16),
            pltpu.VMEM((2, seq, dim), jnp.bfloat16),
            pltpu.VMEM((2, tok_rows, dim), jnp.float32),
            pltpu.VMEM((2, tok_rows, dim), jnp.float32),
            pltpu.VMEM((dim, seq), jnp.float32),
            pltpu.VMEM((dim, seq), jnp.float32),
        ],
        input_output_aliases={5 + i: i for i in range(len(buffers))},
        cost_estimate=pl.CostEstimate(flops=12 * pairs * dim, bytes_accessed=n_batch * 5 * 2 ** 20,
                                      transcendentals=pairs),
        compiler_params=pltpu.CompilerParams(vmem_limit_bytes=60 * 2 ** 20),
    )(query, grad_out, cos_t, sin_t, kv_all, *buffers)


def solution(mesh):
    cp_size = mesh.shape['cp']
    head_spec = P(None, 'cp', 'tp', None)
    pos_spec = P(None, 'cp')

    def local_step(query, keys, values, positions, grad_out):
        batch, length, n_heads, dim = query.shape
        lanes = jnp.arange(dim, dtype=jnp.int32)
        freq_expo = (lanes // 2).astype(jnp.float32) * (2.0 / dim)
        inv_freq = 1.0 / (ROPE_THETA ** freq_expo)
        angles = positions.astype(jnp.float32)[:, :, None] * inv_freq
        cos_t = jnp.cos(angles)
        sin_t = jnp.sin(angles) * jnp.where(lanes % 2 == 0, -1.0, 1.0)
        swap_mat = (lanes[:, None] == (lanes ^ 1)[None, :]).astype(jnp.bfloat16)
        k_t = keys.transpose(2, 0, 1, 3)
        k_swap = jnp.einsum('hbtd,de->hbte', k_t, swap_mat, preferred_element_type=jnp.float32)
        k_rot = (k_t.astype(jnp.float32) * cos_t + k_swap * sin_t).astype(jnp.bfloat16)
        kv = jnp.stack([k_rot, values.transpose(2, 0, 1, 3)])
        n_batch = batch // N_CHUNKS
        gathered = [lax.all_gather(kv[:, :, c * n_batch:(c + 1) * n_batch], 'cp', axis=0) for c in range(N_CHUNKS)]
        buffers = ()
        sums = []
        for c in range(N_CHUNKS):
            *buffers, dkv = attention_chunk(query, grad_out, cos_t, sin_t, gathered[c], buffers, c * n_batch, cp_size)
            sums.append(lax.psum_scatter(dkv, 'cp', scatter_dimension=0, tiled=False))
        total = jnp.concatenate(sums, axis=2)
        dk_rot = total[0]
        dk_swap = jnp.where(lanes % 2 == 0, jnp.roll(dk_rot, -1, axis=-1), jnp.roll(dk_rot, 1, axis=-1))
        grad_keys = (dk_rot * cos_t - dk_swap * sin_t).astype(jnp.bfloat16).transpose(1, 2, 0, 3)
        grad_values = total[1].astype(jnp.bfloat16).transpose(1, 2, 0, 3)
        return buffers[0], buffers[1], grad_keys, grad_values

    return jax.shard_map(local_step, mesh=mesh,
                         in_specs=(head_spec, head_spec, head_spec, pos_spec, head_spec),
                         out_specs=(head_spec, head_spec, head_spec, head_spec), check_vma=False)
```

```python
import functools

import jax
import jax.numpy as jnp
from jax import lax
from jax.experimental import pallas as pl
from jax.experimental.pallas import tpu as pltpu
from jax.sharding import PartitionSpec as P

ROPE_THETA = 1000000.0
LOG2E = 1.4426950408889634
MESH = pl.DeviceIdType.MESH
CP = 8
PIECE = 64
GROUP = 8
DIM = 128
PARTS = 4
LAG_ADD = 3
LAG_END = 5
KEY_BLOCK = 256


def swap_pairs(x):
    lane = lax.broadcasted_iota(jnp.int32, x.shape, 1)
    return jnp.where(lane % 2 == 0, pltpu.roll(x, 127, 1), pltpu.roll(x, 1, 1))


def dot_nt(a, b):
    return lax.dot_general(a, b, (((1,), (1,)), ((), ())), preferred_element_type=jnp.float32)


def dot_nn(a, b):
    return lax.dot_general(a, b, (((1,), (0,)), ((), ())), preferred_element_type=jnp.float32)


def attend_tile(qr, gr, k_view, v_view, n_keys, q_start, scale):
    n_blk = n_keys // KEY_BLOCK
    scores = []
    for j in range(n_blk):
        s = dot_nt(qr, k_view[j * KEY_BLOCK:(j + 1) * KEY_BLOCK, :])
        if j == n_blk - 1:
            q_idx = q_start + lax.broadcasted_iota(jnp.int32, s.shape, 0) // GROUP
            k_idx = j * KEY_BLOCK + lax.broadcasted_iota(jnp.int32, s.shape, 1)
            s = jnp.where(k_idx <= q_idx, s, -jnp.inf)
        scores.append(s)
    row_max = jnp.max(functools.reduce(jnp.maximum, scores), axis=1, keepdims=True)
    expo = [jnp.exp2((s - row_max) * (scale * LOG2E)) for s in scores]
    row_sum = jnp.sum(functools.reduce(jnp.add, expo), axis=1, keepdims=True)
    inv = 1.0 / row_sum
    probs = [e * inv for e in expo]
    p_all = jnp.concatenate([p.astype(jnp.bfloat16) for p in probs], axis=1)
    out = dot_nn(p_all, v_view[0:n_keys, :])
    delta = jnp.sum(out * gr.astype(jnp.float32), axis=1, keepdims=True)
    ds = []
    for j in range(n_blk):
        dp = dot_nt(gr, v_view[j * KEY_BLOCK:(j + 1) * KEY_BLOCK, :])
        ds.append((probs[j] * (dp - delta)).astype(jnp.bfloat16))
    ds_all = jnp.concatenate(ds, axis=1)
    dq = dot_nn(ds_all, k_view[0:n_keys, :]) * scale
    dv_t = dot_nn(gr.T, p_all)
    dk_t = dot_nn(qr.T, ds_all) * scale
    return out, dq, dk_t, dv_t


def fused_kernel(n_batch, q_hbm, g_hbm, cs_hbm, kv_hbm, out_hbm, dq_hbm, dkv_hbm,
                 q_l, g_l, cs_l, kv_l, s1_l, s2_l, part, o_st, f_st, k_s, v_s,
                 kv_loc, kv_send, kv_recv, q_loc, q_send, q_recv, s1_send, s1_recv, s2_send, s2_recv,
                 o_loc, o_send, o_recv, f_loc, f_send, f_recv):
    me = lax.axis_index('cp')
    chip, core = me // 2, me % 2
    sibling = chip * 2 + 1 - core
    n_groups = n_batch // 2
    scale = DIM ** -0.5
    diag = 3 - chip

    def own_slot(half):
        return core if half == 0 else 3 - core

    def sib_slot(half):
        return 1 - core if half == 0 else 2 + core

    def partners(b):
        along_x = chip + 1 - 2 * (chip % 2)
        along_y = (chip + 2) % 4
        odd = b % 2
        return along_x * (1 - odd) + along_y * odd, along_y * (1 - odd) + along_x * odd

    def remote(src, dst, send, recv, device):
        return pltpu.make_async_remote_copy(src_ref=src, dst_ref=dst, send_sem=send, recv_sem=recv,
                                            device_id={'cp': device}, device_id_type=MESH)

    def kv_piece(device, half):
        return device if half == 0 else 2 * CP - 1 - device

    def kv_copy(g, dest, half):
        pair = pl.ds(g * 2, 2)
        return remote(kv_hbm.at[dest % 2, half, pair], kv_l.at[kv_piece(me, half), pair],
                      kv_send.at[g, dest, half], kv_recv.at[g, me, half], dest)

    def kv_own(g, half):
        pair = pl.ds(g * 2, 2)
        return pltpu.make_async_copy(kv_hbm.at[core, half, pair], kv_l.at[kv_piece(me, half), pair], kv_loc.at[g, half])

    def kv_arrive(g, source, half):
        pair = pl.ds(g * 2, 2)
        return remote(kv_hbm.at[core, half, pair], kv_l.at[kv_piece(source, half), pair],
                      kv_send.at[g, source, half], kv_recv.at[g, source, half], source)

    def kv_issue(g):
        for half in range(2):
            kv_own(g, half).start()
        for step in range(1, CP):
            dest = (me + step) % CP
            kv_copy(g, dest, 0).start()

            @pl.when(dest // 2 <= chip)
            def _():
                kv_copy(g, dest, 1).start()

    def kv_wait(g):
        for half in range(2):
            kv_own(g, half).wait()
        for step in range(1, CP):
            source = (me + step) % CP
            kv_arrive(g, source, 0).wait_recv()

            @pl.when(chip <= source // 2)
            def _():
                kv_arrive(g, source, 1).wait_recv()

    def kv_drain(g):
        for step in range(1, CP):
            dest = (me + step) % CP
            kv_copy(g, dest, 0).wait_send()

            @pl.when(dest // 2 <= chip)
            def _():
                kv_copy(g, dest, 1).wait_send()

    def q_views(g, half, slot, head):
        pair = pl.ds(g * 2, 2)
        ring = g % 4
        return ((q_hbm.at[pair, half, :, head], q_l.at[ring, slot]),
                (g_hbm.at[pair, half, :, head], g_l.at[ring, slot]),
                (cs_hbm.at[half, pair], cs_l.at[slot, pair]))

    def q_local(g):
        return [pltpu.make_async_copy(src, dst, q_loc.at[g, i, half]) for half in range(2)
                for i, (src, dst) in enumerate(q_views(g, half, own_slot(half), core))]

    def q_out(g):
        return [remote(src, dst, q_send.at[g, i, half], q_recv.at[g, i, half], sibling) for half in range(2)
                for i, (src, dst) in enumerate(q_views(g, half, own_slot(half), 1 - core))]

    def q_arriving(g):
        return [remote(src, dst, q_send.at[g, i, half], q_recv.at[g, i, half], sibling) for half in range(2)
                for i, (src, dst) in enumerate(q_views(g, half, sib_slot(half), core))]

    def q_issue(g):
        for copy in q_local(g) + q_out(g):
            copy.start()

    def q_wait(g):
        for copy in q_local(g):
            copy.wait()
        for copy in q_arriving(g):
            copy.wait_recv()

    def o_local(b):
        return [pltpu.make_async_copy(o_st.at[b % 2, a, own_slot(half)], ref.at[b, half, :, core],
                                      o_loc.at[b % 2, a, half])
                for a, ref in enumerate((out_hbm, dq_hbm)) for half in range(2)]

    def o_out(b):
        return [remote(o_st.at[b % 2, a, sib_slot(half)], ref.at[b, half, :, core],
                       o_send.at[b % 2, a, half], o_recv.at[b, a, half], sibling)
                for a, ref in enumerate((out_hbm, dq_hbm)) for half in range(2)]

    def o_drain(b):
        for copy in o_local(b):
            copy.wait()
        for copy in o_out(b):
            copy.wait_send()

    def o_wait(b):
        for a, ref in enumerate((out_hbm, dq_hbm)):
            for half in range(2):
                remote(o_st.at[b % 2, a, own_slot(half)], ref.at[b, half, :, 1 - core],
                       o_send.at[b % 2, a, half], o_recv.at[b, a, half], sibling).wait_recv()

    def f_local(b):
        return [pltpu.make_async_copy(f_st.at[b % 2, :, own_slot(half)], dkv_hbm.at[:, core, b, half],
                                      f_loc.at[b % 2, half]) for half in range(2)]

    def f_out(b):
        return [remote(f_st.at[b % 2, :, sib_slot(half)], dkv_hbm.at[:, core, b, half],
                       f_send.at[b % 2, half], f_recv.at[b, half], sibling) for half in range(2)]

    def f_drain(b):
        for copy in f_local(b):
            copy.wait()
        for copy in f_out(b):
            copy.wait_send()

    def f_wait(b):
        for half in range(2):
            remote(f_st.at[b % 2, :, own_slot(half)], dkv_hbm.at[:, 1 - core, b, half],
                   f_send.at[b % 2, half], f_recv.at[b, half], sibling).wait_recv()

    def s1_copy(b, m):
        first, _ = partners(b)
        target = first if m < 2 else diag
        block = target if m % 2 == 0 else 7 - target
        return remote(part.at[b % PARTS, :, block], s1_l.at[b, m], s1_send.at[b % PARTS, m], s1_recv.at[b, m],
                      first * 2 + core)

    def s1_each(b, do):
        first, _ = partners(b)
        for m in range(4):
            if m % 2 == 0:
                do(s1_copy(b, m))
            else:
                target = first if m < 2 else diag

                @pl.when(target > chip)
                def _():
                    do(s1_copy(b, m))

    def s2_copy(b, m):
        _, second = partners(b)
        return remote(s1_l.at[b, 2 + m], s2_l.at[b, m], s2_send.at[b, m], s2_recv.at[b, m], second * 2 + core)

    def s2_send_high(b):
        first, second = partners(b)
        return jnp.logical_or(second > chip, second > first)

    def s2_recv_high(b):
        _, second = partners(b)
        return jnp.logical_or(chip > second, chip > diag)

    def s2_each(b, do):
        do(s2_copy(b, 0))

        @pl.when(s2_send_high(b))
        def _():
            do(s2_copy(b, 1))

    def add_step(b):
        first, second = partners(b)
        ring = b % PARTS
        s1_copy(b, 0).wait_recv()
        s1_copy(b, 2).wait_recv()

        @pl.when(chip > first)
        def _():
            s1_copy(b, 1).wait_recv()

        @pl.when(second > first)
        def _():
            s1_copy(b, 3).wait_recv()

        for i in range(2):
            s1_l[b, 0, i] = s1_l[b, 0, i] + part[ring, i, chip]
            s1_l[b, 2, i] = s1_l[b, 2, i] + part[ring, i, second]
            s1_l[b, 1, i] = jnp.where(chip > first, s1_l[b, 1, i], 0.0) + part[ring, i, 7 - chip]
            s1_l[b, 3, i] = jnp.where(second > first, s1_l[b, 3, i], 0.0) + part[ring, i, 7 - second]

    def end_step(b):
        s2_copy(b, 0).wait_recv()
        has_high = s2_recv_high(b)

        @pl.when(has_high)
        def _():
            s2_copy(b, 1).wait_recv()

        @pl.when(b >= 2)
        def _():
            f_drain(b - 2)

        ring = b % 2
        for m in range(2):
            for i in range(2):
                other = s2_l[b, m, i]
                if m == 1:
                    other = jnp.where(has_high, other, 0.0)
                total = (s1_l[b, m, i] + other).T
                for sub in range(2):
                    slot = m * 2 + sub
                    x = total[sub * PIECE:(sub + 1) * PIECE]
                    if i == 0:
                        x = x * cs_l[slot, b, 0] - swap_pairs(x) * cs_l[slot, b, 1]
                    f_st[ring, i, slot] = x.astype(jnp.bfloat16)

    def compute(b):
        ring, g_ring, b_in = b % PARTS, (b // 2) % 4, b % 2

        @pl.when(b >= PARTS)
        def _():
            s1_each(b - PARTS, lambda copy: copy.wait_send())

        @pl.when(b >= 2)
        def _():
            o_drain(b - 2)

        for piece in range(2 * CP):
            k_p, v_p = kv_l[piece, b, 0], kv_l[piece, b, 1]
            if piece >= CP:
                needed = (2 * CP - 1 - piece) // 2 >= chip
                k_p, v_p = jnp.where(needed, k_p, 0), jnp.where(needed, v_p, 0)
            k_s[piece * PIECE:(piece + 1) * PIECE, :] = k_p.astype(jnp.bfloat16)
            v_s[piece * PIECE:(piece + 1) * PIECE, :] = v_p.astype(jnp.bfloat16)
        for i in range(2):
            for j in range(8):
                part[ring, i, j] = jnp.zeros((DIM, DIM), jnp.float32)

        def tile(slot, n_keys, q_start):
            rows = PIECE * GROUP
            cos = jnp.broadcast_to(cs_l[slot, b, 0][:, None, :], (PIECE, GROUP, DIM)).reshape(rows, DIM)
            sin = jnp.broadcast_to(cs_l[slot, b, 1][:, None, :], (PIECE, GROUP, DIM)).reshape(rows, DIM)
            qx = q_l[g_ring, slot, b_in].astype(jnp.float32).reshape(rows, DIM)
            qr = (qx * cos + swap_pairs(qx) * sin).astype(jnp.bfloat16)
            gr = g_l[g_ring, slot, b_in].astype(jnp.float32).reshape(rows, DIM).astype(jnp.bfloat16)
            out, dq, dk_t, dv_t = attend_tile(qr, gr, k_s, v_s, n_keys, q_start, scale)
            dq = dq * cos - swap_pairs(dq) * sin
            o_st[b % 2, 0, slot] = out.reshape(PIECE, GROUP, DIM).astype(jnp.bfloat16)
            o_st[b % 2, 1, slot] = dq.reshape(PIECE, GROUP, DIM).astype(jnp.bfloat16)
            for j in range(n_keys // DIM):
                part[ring, 0, j] += dk_t[:, j * DIM:(j + 1) * DIM]
                part[ring, 1, j] += dv_t[:, j * DIM:(j + 1) * DIM]

        def variant(n_low, n_high):
            def high(i, carry):
                tile(2 + i, n_high, (2 * CP - 2 - 2 * chip + i) * PIECE)
                return carry

            def low(i, carry):
                tile(i, n_low, (2 * chip + i) * PIECE)
                return carry

            lax.fori_loop(0, 2, high, 0)
            lax.fori_loop(0, 2, low, 0)

        @pl.when(chip < 2)
        def _():
            variant(CP * PIECE // 2, 2 * CP * PIECE)

        @pl.when(chip >= 2)
        def _():
            variant(CP * PIECE, CP * PIECE * 3 // 2)

    barrier = pltpu.get_barrier_semaphore()
    for step in range(1, CP):
        pl.semaphore_signal(barrier, inc=1, device_id={'cp': (me + step) % CP}, device_id_type=MESH)
    pl.semaphore_wait(barrier, CP - 1)

    for g in range(2):
        kv_issue(g)
        q_issue(g)

    def step(it, carry):
        even = it % 2 == 0

        @pl.when(jnp.logical_and(even, jnp.logical_and(it >= 4, it + 4 < n_batch)))
        def _():
            o_wait(it - 4)
            o_wait(it - 3)

        @pl.when(jnp.logical_and(even, it + 4 < n_batch))
        def _():
            kv_issue(it // 2 + 2)
            q_issue(it // 2 + 2)

        @pl.when(jnp.logical_and(it >= LAG_ADD, it < n_batch + LAG_ADD))
        def _():
            add_step(it - LAG_ADD)

        @pl.when(it >= LAG_END)
        def _():
            end_step(it - LAG_END)

        @pl.when(jnp.logical_and(it >= LAG_ADD, it < n_batch + LAG_ADD))
        def _():
            s2_each(it - LAG_ADD, lambda copy: copy.start())

        @pl.when(jnp.logical_and(even, it < n_batch))
        def _():
            kv_wait(it // 2)
            q_wait(it // 2)

        @pl.when(it < n_batch)
        def _():
            compute(it)
            s1_each(it, lambda copy: copy.start())
            for copy in o_local(it) + o_out(it):
                copy.start()

        @pl.when(it >= LAG_END)
        def _():
            for copy in f_local(it - LAG_END) + f_out(it - LAG_END):
                copy.start()

        return carry

    lax.fori_loop(0, n_batch + LAG_END, step, 0)

    for b in range(n_batch - PARTS, n_batch):
        s1_each(b, lambda copy: copy.wait_send())
    for b in range(n_batch - 2, n_batch):
        o_drain(b)
        f_drain(b)

    def drain_group(g, carry):
        kv_drain(g)
        for copy in q_out(g):
            copy.wait_send()
        return carry

    def drain_batch(b, carry):
        s2_each(b, lambda copy: copy.wait_send())
        f_wait(b)
        return carry

    def drain_out(b, carry):
        o_wait(b)
        return carry

    lax.fori_loop(0, n_groups, drain_group, 0)
    lax.fori_loop(0, n_batch, drain_batch, 0)
    lax.fori_loop(n_batch - 8, n_batch, drain_out, 0)


def fused_attention(query, grad_out, tables, kv):
    n_batch = query.shape[0]
    n_groups = n_batch // 2
    sem = pltpu.SemaphoreType.DMA
    f32, bf16 = jnp.float32, jnp.bfloat16
    any_spec = pl.BlockSpec(memory_space=pl.ANY)
    return pl.pallas_call(
        functools.partial(fused_kernel, n_batch),
        out_shape=(jax.ShapeDtypeStruct(query.shape, bf16), jax.ShapeDtypeStruct(query.shape, bf16),
                   jax.ShapeDtypeStruct((2, 2, n_batch, 2, PIECE, DIM), bf16)),
        in_specs=[any_spec] * 4,
        out_specs=(any_spec,) * 3,
        scratch_shapes=[
            pltpu.VMEM((4, 4, 2, PIECE, GROUP, DIM), bf16),
            pltpu.VMEM((4, 4, 2, PIECE, GROUP, DIM), bf16),
            pltpu.VMEM((4, n_batch, 2, PIECE, DIM), f32),
            pltpu.VMEM((2 * CP, n_batch, 2, PIECE, DIM), bf16),
            pltpu.VMEM((n_batch, 4, 2, DIM, DIM), f32),
            pltpu.VMEM((n_batch, 2, 2, DIM, DIM), f32),
            pltpu.VMEM((PARTS, 2, 8, DIM, DIM), f32),
            pltpu.VMEM((2, 2, 4, PIECE, GROUP, DIM), bf16),
            pltpu.VMEM((2, 2, 4, PIECE, DIM), bf16),
            pltpu.VMEM((2 * CP * PIECE, DIM), bf16),
            pltpu.VMEM((2 * CP * PIECE, DIM), bf16),
            sem((n_groups, 2)), sem((n_groups, CP, 2)), sem((n_groups, CP, 2)),
            sem((n_groups, 3, 2)), sem((n_groups, 3, 2)), sem((n_groups, 3, 2)),
            sem((PARTS, 4)), sem((n_batch, 4)), sem((n_batch, 2)), sem((n_batch, 2)),
            sem((2, 2, 2)), sem((2, 2, 2)), sem((n_batch, 2, 2)),
            sem((2, 2)), sem((2, 2)), sem((n_batch, 2)),
        ],
        compiler_params=pltpu.CompilerParams(collective_id=0, has_side_effects=True, vmem_limit_bytes=67043328),
    )(query, grad_out, tables, kv)


def solution(mesh):
    head_spec = P(None, 'cp', 'tp', None)
    pos_spec = P(None, 'cp')

    def local_step(query, keys, values, positions, grad_out):
        batch, length, n_heads, dim = query.shape
        lanes = jnp.arange(dim, dtype=jnp.int32)
        freq_expo = (lanes // 2).astype(jnp.float32) * (2.0 / dim)
        inv_freq = 1.0 / (ROPE_THETA ** freq_expo)
        angles = positions.astype(jnp.float32)[:, :, None] * inv_freq
        cos_t = jnp.cos(angles)
        sin_t = jnp.sin(angles) * jnp.where(lanes % 2 == 0, -1.0, 1.0)
        swap_mat = (lanes[:, None] == (lanes ^ 1)[None, :]).astype(jnp.bfloat16)
        k_t = keys.transpose(2, 0, 1, 3)
        k_swap = jnp.einsum('hbtd,de->hbte', k_t, swap_mat, preferred_element_type=jnp.float32)
        k_rot = (k_t.astype(jnp.float32) * cos_t + k_swap * sin_t).astype(jnp.bfloat16)
        by_half = (2, batch, 2, PIECE, dim)
        kv = jnp.stack([k_rot.reshape(by_half), values.transpose(2, 0, 1, 3).reshape(by_half)], axis=3)
        kv = kv.transpose(0, 2, 1, 3, 4, 5)
        tables = jnp.stack([cos_t.reshape(by_half[1:]), sin_t.reshape(by_half[1:])], axis=2).transpose(1, 0, 2, 3, 4)
        split = (batch, 2, PIECE, 2, GROUP, dim)
        out, dq, dkv = fused_attention(query.reshape(split), grad_out.reshape(split), tables, kv)
        dkv = dkv.reshape(2, 2, batch, length, dim).transpose(0, 2, 3, 1, 4)
        return out.reshape(query.shape), dq.reshape(query.shape), dkv[0], dkv[1]

    return jax.shard_map(local_step, mesh=mesh,
                         in_specs=(head_spec, head_spec, head_spec, pos_spec, head_spec),
                         out_specs=(head_spec, head_spec, head_spec, head_spec), check_vma=False)
```

```python
import functools
import math

import jax
import jax.numpy as jnp
from jax import lax
from jax.experimental import pallas as pl
from jax.experimental.pallas import tpu as pltpu
from jax.sharding import PartitionSpec as P

ROPE_THETA = 1000000.0
LOG2E = 1.4426950408889634
MESH = pl.DeviceIdType.MESH
CP = 8
PIECE = 64
GROUP = 8
DIM = 128
PARTS = 4
LAG_ADD = 3
LAG_END = 5
KEY_BLOCK = 256
AHEAD = 4


def swap_pairs(x):
    lane = lax.broadcasted_iota(jnp.int32, x.shape, 1)
    return jnp.where(lane % 2 == 0, pltpu.roll(x, 127, 1), pltpu.roll(x, 1, 1))


def dot_nt(a, b):
    return lax.dot_general(a, b, (((1,), (1,)), ((), ())), preferred_element_type=jnp.float32)


def dot_nn(a, b):
    return lax.dot_general(a, b, (((1,), (0,)), ((), ())), preferred_element_type=jnp.float32)


def attend_tile(qr, gr, k_view, v_view, n_keys, q_start, scale):
    n_blk = n_keys // KEY_BLOCK
    scores = []
    for j in range(n_blk):
        s = dot_nt(qr, k_view[j * KEY_BLOCK:(j + 1) * KEY_BLOCK, :])
        if j == n_blk - 1:
            q_idx = q_start + lax.broadcasted_iota(jnp.int32, s.shape, 0) // GROUP
            k_idx = j * KEY_BLOCK + lax.broadcasted_iota(jnp.int32, s.shape, 1)
            s = jnp.where(k_idx <= q_idx, s, -jnp.inf)
        scores.append(s)
    row_max = jnp.max(functools.reduce(jnp.maximum, scores), axis=1, keepdims=True)
    expo = [jnp.exp2((s - row_max) * (scale * LOG2E)) for s in scores]
    row_sum = jnp.sum(functools.reduce(jnp.add, expo), axis=1, keepdims=True)
    inv = 1.0 / row_sum
    probs = [e * inv for e in expo]
    p_all = jnp.concatenate([p.astype(jnp.bfloat16) for p in probs], axis=1)
    out = dot_nn(p_all, v_view[0:n_keys, :])
    delta = jnp.sum(out * gr.astype(jnp.float32), axis=1, keepdims=True)
    ds = []
    for j in range(n_blk):
        dp = dot_nt(gr, v_view[j * KEY_BLOCK:(j + 1) * KEY_BLOCK, :])
        ds.append((probs[j] * (dp - delta)).astype(jnp.bfloat16))
    ds_all = jnp.concatenate(ds, axis=1)
    dq = dot_nn(ds_all, k_view[0:n_keys, :]) * scale
    dv_t = dot_nn(gr.T, p_all)
    dk_t = dot_nn(qr.T, ds_all) * scale
    return out, dq, dk_t, dv_t


def fused_kernel(n_batch, q_hbm, g_hbm, cs_hbm, kv_hbm, out_hbm, dq_hbm, dk_hbm, dv_hbm,
                 q_l, g_l, cs_l, kv_l, s1_l, s2_l, part, o_st, f_st, k_s, v_s,
                 kv_loc, kv_send, kv_recv, q_loc, q_send, q_recv, s1_send, s1_recv, s2_send, s2_recv,
                 o_loc, o_send, o_recv, f_loc, f_send, f_recv):
    me = lax.axis_index('cp')
    chip, core = me // 2, me % 2
    sibling = chip * 2 + 1 - core
    n_groups = n_batch // 2
    scale = DIM ** -0.5
    diag = 3 - chip

    def own_slot(half):
        return core if half == 0 else 3 - core

    def sib_slot(half):
        return 1 - core if half == 0 else 2 + core

    def partners(b):
        along_x = chip + 1 - 2 * (chip % 2)
        along_y = (chip + 2) % 4
        odd = b % 2
        return along_x * (1 - odd) + along_y * odd, along_y * (1 - odd) + along_x * odd

    def remote(src, dst, send, recv, device):
        return pltpu.make_async_remote_copy(src_ref=src, dst_ref=dst, send_sem=send, recv_sem=recv,
                                            device_id={'cp': device}, device_id_type=MESH)

    def kv_piece(device, half):
        return device if half == 0 else 2 * CP - 1 - device

    def kv_copy(g, dest, half):
        pair = pl.ds(g * 2, 2)
        return remote(kv_hbm.at[dest % 2, half, pair], kv_l.at[kv_piece(me, half), pair],
                      kv_send.at[g, dest, half], kv_recv.at[g, me, half], dest)

    def kv_own(g, half):
        pair = pl.ds(g * 2, 2)
        return pltpu.make_async_copy(kv_hbm.at[core, half, pair], kv_l.at[kv_piece(me, half), pair], kv_loc.at[g, half])

    def kv_arrive(g, source, half):
        pair = pl.ds(g * 2, 2)
        return remote(kv_hbm.at[core, half, pair], kv_l.at[kv_piece(source, half), pair],
                      kv_send.at[g, source, half], kv_recv.at[g, source, half], source)

    def kv_issue(g):
        for half in range(2):
            kv_own(g, half).start()
        for step in range(1, CP):
            dest = (me + step) % CP
            kv_copy(g, dest, 0).start()

            @pl.when(dest // 2 <= chip)
            def _():
                kv_copy(g, dest, 1).start()

    def kv_wait(g):
        for half in range(2):
            kv_own(g, half).wait()
        for step in range(1, CP):
            source = (me + step) % CP
            kv_arrive(g, source, 0).wait_recv()

            @pl.when(chip <= source // 2)
            def _():
                kv_arrive(g, source, 1).wait_recv()

    def kv_drain(g):
        for step in range(1, CP):
            dest = (me + step) % CP
            kv_copy(g, dest, 0).wait_send()

            @pl.when(dest // 2 <= chip)
            def _():
                kv_copy(g, dest, 1).wait_send()

    def q_views(g, half, slot, head):
        pair = pl.ds(g * 2, 2)
        ring = g % 4
        return ((q_hbm.at[pair, half, :, head], q_l.at[ring, slot]),
                (g_hbm.at[pair, half, :, head], g_l.at[ring, slot]),
                (cs_hbm.at[half, pair], cs_l.at[slot, pair]))

    def q_local(g):
        return [pltpu.make_async_copy(src, dst, q_loc.at[g, i, half]) for half in range(2)
                for i, (src, dst) in enumerate(q_views(g, half, own_slot(half), core))]

    def q_out(g):
        return [remote(src, dst, q_send.at[g, i, half], q_recv.at[g, i, half], sibling) for half in range(2)
                for i, (src, dst) in enumerate(q_views(g, half, own_slot(half), 1 - core))]

    def q_arriving(g):
        return [remote(src, dst, q_send.at[g, i, half], q_recv.at[g, i, half], sibling) for half in range(2)
                for i, (src, dst) in enumerate(q_views(g, half, sib_slot(half), core))]

    def q_issue(g):
        for copy in q_local(g) + q_out(g):
            copy.start()

    def q_wait(g):
        for copy in q_local(g):
            copy.wait()
        for copy in q_arriving(g):
            copy.wait_recv()

    def o_local(b):
        return [pltpu.make_async_copy(o_st.at[b % 2, a, own_slot(half)], ref.at[b, half, :, core],
                                      o_loc.at[b % 2, a, half])
                for a, ref in enumerate((out_hbm, dq_hbm)) for half in range(2)]

    def o_out(b):
        return [remote(o_st.at[b % 2, a, sib_slot(half)], ref.at[b, half, :, core],
                       o_send.at[b % 2, a, half], o_recv.at[b, a, half], sibling)
                for a, ref in enumerate((out_hbm, dq_hbm)) for half in range(2)]

    def o_drain(b):
        for copy in o_local(b):
            copy.wait()
        for copy in o_out(b):
            copy.wait_send()

    def o_wait(b):
        for a, ref in enumerate((out_hbm, dq_hbm)):
            for half in range(2):
                remote(o_st.at[b % 2, a, own_slot(half)], ref.at[b, half, :, 1 - core],
                       o_send.at[b % 2, a, half], o_recv.at[b, a, half], sibling).wait_recv()

    def f_local(b):
        return [pltpu.make_async_copy(f_st.at[b % 2, a, own_slot(half)], ref.at[core, b, half], f_loc.at[b % 2, a, half])
                for a, ref in enumerate((dk_hbm, dv_hbm)) for half in range(2)]

    def f_out(b):
        return [remote(f_st.at[b % 2, a, sib_slot(half)], ref.at[core, b, half],
                       f_send.at[b % 2, a, half], f_recv.at[b, a, half], sibling)
                for a, ref in enumerate((dk_hbm, dv_hbm)) for half in range(2)]

    def f_drain(b):
        for copy in f_local(b):
            copy.wait()
        for copy in f_out(b):
            copy.wait_send()

    def f_wait(b):
        for a, ref in enumerate((dk_hbm, dv_hbm)):
            for half in range(2):
                remote(f_st.at[b % 2, a, own_slot(half)], ref.at[1 - core, b, half],
                       f_send.at[b % 2, a, half], f_recv.at[b, a, half], sibling).wait_recv()

    def s1_copy(b, m):
        first, _ = partners(b)
        target = first if m < 2 else diag
        block = target if m % 2 == 0 else 7 - target
        return remote(part.at[b % PARTS, :, block], s1_l.at[b, m], s1_send.at[b % PARTS, m], s1_recv.at[b, m],
                      first * 2 + core)

    def s1_each(b, do):
        first, _ = partners(b)
        for m in range(4):
            if m % 2 == 0:
                do(s1_copy(b, m))
            else:
                target = first if m < 2 else diag

                @pl.when(target > chip)
                def _():
                    do(s1_copy(b, m))

    def s2_copy(b, m):
        _, second = partners(b)
        return remote(s1_l.at[b, 2 + m], s2_l.at[b, m], s2_send.at[b, m], s2_recv.at[b, m], second * 2 + core)

    def s2_send_high(b):
        first, second = partners(b)
        return jnp.logical_or(second > chip, second > first)

    def s2_recv_high(b):
        _, second = partners(b)
        return jnp.logical_or(chip > second, chip > diag)

    def s2_each(b, do):
        do(s2_copy(b, 0))

        @pl.when(s2_send_high(b))
        def _():
            do(s2_copy(b, 1))

    def add_step(b):
        first, second = partners(b)
        ring = b % PARTS
        s1_copy(b, 0).wait_recv()
        s1_copy(b, 2).wait_recv()

        @pl.when(chip > first)
        def _():
            s1_copy(b, 1).wait_recv()

        @pl.when(second > first)
        def _():
            s1_copy(b, 3).wait_recv()

        for i in range(2):
            s1_l[b, 0, i] = s1_l[b, 0, i] + part[ring, i, chip]
            s1_l[b, 2, i] = s1_l[b, 2, i] + part[ring, i, second]
            s1_l[b, 1, i] = jnp.where(chip > first, s1_l[b, 1, i], 0.0) + part[ring, i, 7 - chip]
            s1_l[b, 3, i] = jnp.where(second > first, s1_l[b, 3, i], 0.0) + part[ring, i, 7 - second]

    def end_step(b):
        s2_copy(b, 0).wait_recv()
        has_high = s2_recv_high(b)

        @pl.when(has_high)
        def _():
            s2_copy(b, 1).wait_recv()

        @pl.when(b >= 2)
        def _():
            f_drain(b - 2)

        ring = b % 2
        for m in range(2):
            for i in range(2):
                other = s2_l[b, m, i]
                if m == 1:
                    other = jnp.where(has_high, other, 0.0)
                total = (s1_l[b, m, i] + other).T
                for sub in range(2):
                    slot = m * 2 + sub
                    x = total[sub * PIECE:(sub + 1) * PIECE]
                    if i == 0:
                        x = x * cs_l[slot, b, 0] - swap_pairs(x) * cs_l[slot, b, 1]
                    f_st[ring, i, slot] = x.astype(jnp.bfloat16)

    def compute(b):
        ring, g_ring, b_in = b % PARTS, (b // 2) % 4, b % 2

        @pl.when(b >= PARTS)
        def _():
            s1_each(b - PARTS, lambda copy: copy.wait_send())

        @pl.when(b >= 2)
        def _():
            o_drain(b - 2)

        for piece in range(2 * CP):
            k_p, v_p = kv_l[piece, b, 0], kv_l[piece, b, 1]
            if piece >= CP:
                needed = (2 * CP - 1 - piece) // 2 >= chip
                k_p, v_p = jnp.where(needed, k_p, 0), jnp.where(needed, v_p, 0)
            k_s[piece * PIECE:(piece + 1) * PIECE, :] = k_p.astype(jnp.bfloat16)
            v_s[piece * PIECE:(piece + 1) * PIECE, :] = v_p.astype(jnp.bfloat16)
        for i in range(2):
            for j in range(8):
                part[ring, i, j] = jnp.zeros((DIM, DIM), jnp.float32)

        def tile(slot, n_keys, q_start):
            rows = PIECE * GROUP
            cos = jnp.broadcast_to(cs_l[slot, b, 0][:, None, :], (PIECE, GROUP, DIM)).reshape(rows, DIM)
            sin = jnp.broadcast_to(cs_l[slot, b, 1][:, None, :], (PIECE, GROUP, DIM)).reshape(rows, DIM)
            qx = q_l[g_ring, slot, b_in].astype(jnp.float32).reshape(rows, DIM)
            qr = (qx * cos + swap_pairs(qx) * sin).astype(jnp.bfloat16)
            gr = g_l[g_ring, slot, b_in].astype(jnp.float32).reshape(rows, DIM).astype(jnp.bfloat16)
            out, dq, dk_t, dv_t = attend_tile(qr, gr, k_s, v_s, n_keys, q_start, scale)
            dq = dq * cos - swap_pairs(dq) * sin
            o_st[b % 2, 0, slot] = out.reshape(PIECE, GROUP, DIM).astype(jnp.bfloat16)
            o_st[b % 2, 1, slot] = dq.reshape(PIECE, GROUP, DIM).astype(jnp.bfloat16)
            for j in range(n_keys // DIM):
                part[ring, 0, j] += dk_t[:, j * DIM:(j + 1) * DIM]
                part[ring, 1, j] += dv_t[:, j * DIM:(j + 1) * DIM]

        def variant(n_low, n_high):
            def high(i, carry):
                tile(2 + i, n_high, (2 * CP - 2 - 2 * chip + i) * PIECE)
                return carry

            def low(i, carry):
                tile(i, n_low, (2 * chip + i) * PIECE)
                return carry

            lax.fori_loop(0, 2, high, 0)
            lax.fori_loop(0, 2, low, 0)

        @pl.when(chip < 2)
        def _():
            variant(CP * PIECE // 2, 2 * CP * PIECE)

        @pl.when(chip >= 2)
        def _():
            variant(CP * PIECE, CP * PIECE * 3 // 2)

    barrier = pltpu.get_barrier_semaphore()
    for step in range(1, CP):
        pl.semaphore_signal(barrier, inc=1, device_id={'cp': (me + step) % CP}, device_id_type=MESH)
    pl.semaphore_wait(barrier, CP - 1)

    for g in range(2):
        kv_issue(g)
        q_issue(g)
    for g in range(2, AHEAD):
        kv_issue(g)

    def step(it, carry):
        even = it % 2 == 0

        @pl.when(jnp.logical_and(even, jnp.logical_and(it >= 4, it + 4 < n_batch)))
        def _():
            o_wait(it - 4)
            o_wait(it - 3)

        @pl.when(jnp.logical_and(even, it + 4 < n_batch))
        def _():
            q_issue(it // 2 + 2)

        @pl.when(jnp.logical_and(even, it + 2 * AHEAD < n_batch))
        def _():
            kv_issue(it // 2 + AHEAD)

        @pl.when(jnp.logical_and(it >= LAG_ADD, it < n_batch + LAG_ADD))
        def _():
            add_step(it - LAG_ADD)

        @pl.when(it >= LAG_END)
        def _():
            end_step(it - LAG_END)

        @pl.when(jnp.logical_and(it >= LAG_ADD, it < n_batch + LAG_ADD))
        def _():
            s2_each(it - LAG_ADD, lambda copy: copy.start())

        @pl.when(jnp.logical_and(even, it < n_batch))
        def _():
            kv_wait(it // 2)
            q_wait(it // 2)

        @pl.when(it < n_batch)
        def _():
            compute(it)
            s1_each(it, lambda copy: copy.start())
            for copy in o_local(it) + o_out(it):
                copy.start()

        @pl.when(it >= LAG_END)
        def _():
            for copy in f_local(it - LAG_END) + f_out(it - LAG_END):
                copy.start()

        return carry

    lax.fori_loop(0, n_batch + LAG_END, step, 0)

    for b in range(n_batch - PARTS, n_batch):
        s1_each(b, lambda copy: copy.wait_send())
    for b in range(n_batch - 2, n_batch):
        o_drain(b)
        f_drain(b)

    def drain_group(g, carry):
        kv_drain(g)
        for copy in q_out(g):
            copy.wait_send()
        return carry

    def drain_batch(b, carry):
        s2_each(b, lambda copy: copy.wait_send())
        f_wait(b)
        return carry

    def drain_out(b, carry):
        o_wait(b)
        return carry

    lax.fori_loop(0, n_groups, drain_group, 0)
    lax.fori_loop(0, n_batch, drain_batch, 0)
    lax.fori_loop(n_batch - 8, n_batch, drain_out, 0)


def fused_attention(query, grad_out, tables, kv):
    n_batch = query.shape[0]
    n_groups = n_batch // 2
    sem = pltpu.SemaphoreType.DMA
    f32, bf16 = jnp.float32, jnp.bfloat16
    any_spec = pl.BlockSpec(memory_space=pl.ANY)
    return pl.pallas_call(
        functools.partial(fused_kernel, n_batch),
        out_shape=(jax.ShapeDtypeStruct(query.shape, bf16), jax.ShapeDtypeStruct(query.shape, bf16),
                   jax.ShapeDtypeStruct((2, n_batch, 2, PIECE, DIM), bf16),
                   jax.ShapeDtypeStruct((2, n_batch, 2, PIECE, DIM), bf16)),
        in_specs=[any_spec] * 4,
        out_specs=(any_spec,) * 4,
        scratch_shapes=[
            pltpu.VMEM((4, 4, 2, PIECE, GROUP, DIM), bf16),
            pltpu.VMEM((4, 4, 2, PIECE, GROUP, DIM), bf16),
            pltpu.VMEM((4, n_batch, 2, PIECE, DIM), f32),
            pltpu.VMEM((2 * CP, n_batch, 2, PIECE, DIM), bf16),
            pltpu.VMEM((n_batch, 4, 2, DIM, DIM), f32),
            pltpu.VMEM((n_batch, 2, 2, DIM, DIM), f32),
            pltpu.VMEM((PARTS, 2, 8, DIM, DIM), f32),
            pltpu.VMEM((2, 2, 4, PIECE, GROUP, DIM), bf16),
            pltpu.VMEM((2, 2, 4, PIECE, DIM), bf16),
            pltpu.VMEM((2 * CP * PIECE, DIM), bf16),
            pltpu.VMEM((2 * CP * PIECE, DIM), bf16),
            sem((n_groups, 2)), sem((n_groups, CP, 2)), sem((n_groups, CP, 2)),
            sem((n_groups, 3, 2)), sem((n_groups, 3, 2)), sem((n_groups, 3, 2)),
            sem((PARTS, 4)), sem((n_batch, 4)), sem((n_batch, 2)), sem((n_batch, 2)),
            sem((2, 2, 2)), sem((2, 2, 2)), sem((n_batch, 2, 2)),
            sem((2, 2, 2)), sem((2, 2, 2)), sem((n_batch, 2, 2)),
        ],
        compiler_params=pltpu.CompilerParams(collective_id=0, has_side_effects=True, vmem_limit_bytes=67043328),
    )(query, grad_out, tables, kv)


def copy_kernel(a_ref, b_ref, c_ref, d_ref):
    c_ref[...] = a_ref[...]
    d_ref[...] = b_ref[...]


def copy_results(a, b):
    spec = pl.BlockSpec((1,) + a.shape[1:], lambda i: (i,) + (0,) * (a.ndim - 1))
    return pl.pallas_call(copy_kernel, grid=(a.shape[0],), in_specs=[spec, spec], out_specs=(spec, spec),
                          out_shape=(jax.ShapeDtypeStruct(a.shape, a.dtype), jax.ShapeDtypeStruct(b.shape, b.dtype)))(a, b)


def cos_sin(angles):
    turns = jnp.floor(angles * (2.0 / math.pi) + 0.5)
    rest = ((angles - turns * 1.5703125) - turns * 4.837512969970703125e-4) - turns * 7.549789948768648e-8
    sq = rest * rest
    sine = ((-1.9515295891e-4 * sq + 8.3321608736e-3) * sq - 1.6666654611e-1) * sq * rest + rest
    cosine = ((2.443315711809948e-5 * sq - 1.388731625493765e-3) * sq + 4.166664568298827e-2) * sq * sq - 0.5 * sq + 1.0
    quarter = turns.astype(jnp.int32) % 4
    odd = quarter % 2 == 1
    cos_v = jnp.where(odd, sine, cosine)
    sin_v = jnp.where(odd, cosine, sine)
    cos_v = jnp.where((quarter == 1) | (quarter == 2), -cos_v, cos_v)
    sin_v = jnp.where(quarter >= 2, -sin_v, sin_v)
    return cos_v, sin_v


def solution(mesh):
    head_spec = P(None, 'cp', 'tp', None)
    pos_spec = P(None, 'cp')

    def local_step(query, keys, values, positions, grad_out):
        batch, length, n_heads, dim = query.shape
        lanes = jnp.arange(dim, dtype=jnp.int32)
        freq_expo = (lanes // 2).astype(jnp.float32) * (2.0 / dim)
        inv_freq = 1.0 / (ROPE_THETA ** freq_expo)
        angles = positions.astype(jnp.float32)[:, :, None] * inv_freq
        cos_t, sin_t = cos_sin(angles)
        sin_t = sin_t * jnp.where(lanes % 2 == 0, -1.0, 1.0)
        swap_mat = (lanes[:, None] == (lanes ^ 1)[None, :]).astype(jnp.bfloat16)
        k_t = keys.transpose(2, 0, 1, 3)
        k_swap = jnp.einsum('hbtd,de->hbte', k_t, swap_mat, preferred_element_type=jnp.float32)
        k_rot = (k_t.astype(jnp.float32) * cos_t + k_swap * sin_t).astype(jnp.bfloat16)
        by_half = (2, batch, 2, PIECE, dim)
        kv = jnp.stack([k_rot.reshape(by_half), values.transpose(2, 0, 1, 3).reshape(by_half)], axis=3)
        kv = kv.transpose(0, 2, 1, 3, 4, 5)
        tables = jnp.stack([cos_t.reshape(by_half[1:]), sin_t.reshape(by_half[1:])], axis=2).transpose(1, 0, 2, 3, 4)
        split = (batch, 2, PIECE, 2, GROUP, dim)
        out, dq, dk, dv = fused_attention(query.reshape(split), grad_out.reshape(split), tables, kv)
        out, dq = copy_results(out.reshape(query.shape), dq.reshape(query.shape))
        back = (2, batch, length, dim)
        return out, dq, dk.reshape(back).transpose(1, 2, 0, 3), dv.reshape(back).transpose(1, 2, 0, 3)

    return jax.shard_map(local_step, mesh=mesh,
                         in_specs=(head_spec, head_spec, head_spec, pos_spec, head_spec),
                         out_specs=(head_spec, head_spec, head_spec, head_spec), check_vma=False)
```

```python
import functools
import math

import jax
import jax.numpy as jnp
from jax import lax
from jax.experimental import pallas as pl
from jax.experimental.pallas import tpu as pltpu
from jax.sharding import PartitionSpec as P

ROPE_THETA = 1000000.0
LOG2E = 1.4426950408889634
MESH = pl.DeviceIdType.MESH
CP = 8
PIECE = 64
GROUP = 8
DIM = 128
PARTS = 4
LAG_ADD = 3
LAG_END = 5
KEY_BLOCK = 256
VMEM_MIB = 36
Q_RING = 3
CS_RING = 12
S1_RING = 10
S2_RING = 6


def swap_pairs(x):
    lane = lax.broadcasted_iota(jnp.int32, x.shape, 1)
    return jnp.where(lane % 2 == 0, pltpu.roll(x, 127, 1), pltpu.roll(x, 1, 1))


def dot_nt(a, b):
    return lax.dot_general(a, b, (((1,), (1,)), ((), ())), preferred_element_type=jnp.float32)


def dot_nn(a, b):
    return lax.dot_general(a, b, (((1,), (0,)), ((), ())), preferred_element_type=jnp.float32)


def attend_tile(qr, gr, k_view, v_view, n_keys, q_start, scale):
    n_blk = n_keys // KEY_BLOCK
    scores = []
    for j in range(n_blk):
        s = dot_nt(qr, k_view[j * KEY_BLOCK:(j + 1) * KEY_BLOCK, :])
        if j == n_blk - 1:
            q_idx = q_start + lax.broadcasted_iota(jnp.int32, s.shape, 0) // GROUP
            k_idx = j * KEY_BLOCK + lax.broadcasted_iota(jnp.int32, s.shape, 1)
            s = jnp.where(k_idx <= q_idx, s, -jnp.inf)
        scores.append(s)
    row_max = jnp.max(functools.reduce(jnp.maximum, scores), axis=1, keepdims=True)
    expo = [jnp.exp2((s - row_max) * (scale * LOG2E)) for s in scores]
    row_sum = jnp.sum(functools.reduce(jnp.add, expo), axis=1, keepdims=True)
    inv = 1.0 / row_sum
    probs = [e * inv for e in expo]
    p_all = jnp.concatenate([p.astype(jnp.bfloat16) for p in probs], axis=1)
    out = dot_nn(p_all, v_view[0:n_keys, :])
    delta = jnp.sum(out * gr.astype(jnp.float32), axis=1, keepdims=True)
    ds = []
    for j in range(n_blk):
        dp = dot_nt(gr, v_view[j * KEY_BLOCK:(j + 1) * KEY_BLOCK, :])
        ds.append((probs[j] * (dp - delta)).astype(jnp.bfloat16))
    ds_all = jnp.concatenate(ds, axis=1)
    dq = dot_nn(ds_all, k_view[0:n_keys, :]) * scale
    dv_t = dot_nn(gr.T, p_all)
    dk_t = dot_nn(qr.T, ds_all) * scale
    return out, dq, dk_t, dv_t


def fused_kernel(n_batch, q_hbm, g_hbm, cs_hbm, kv_hbm, out_hbm, dq_hbm, dk_hbm, dv_hbm,
                 q_l, g_l, cs_l, kv_l, s1_l, s2_l, part, o_st, f_st, k_s, v_s,
                 kv_loc, kv_send, kv_recv, q_loc, q_send, q_recv, s1_send, s1_recv, s2_send, s2_recv,
                 o_loc, o_send, o_recv, f_loc, f_send, f_recv):
    me = lax.axis_index('cp')
    chip, core = me // 2, me % 2
    sibling = chip * 2 + 1 - core
    n_groups = n_batch // 2
    scale = DIM ** -0.5
    diag = 3 - chip

    def own_slot(half):
        return core if half == 0 else 3 - core

    def sib_slot(half):
        return 1 - core if half == 0 else 2 + core

    def partners(b):
        along_x = chip + 1 - 2 * (chip % 2)
        along_y = (chip + 2) % 4
        odd = b % 2
        return along_x * (1 - odd) + along_y * odd, along_y * (1 - odd) + along_x * odd

    def remote(src, dst, send, recv, device):
        return pltpu.make_async_remote_copy(src_ref=src, dst_ref=dst, send_sem=send, recv_sem=recv,
                                            device_id={'cp': device}, device_id_type=MESH)

    def kv_piece(device, half):
        return device if half == 0 else 2 * CP - 1 - device

    def kv_copy(g, dest, half):
        pair = pl.ds(g * 2, 2)
        return remote(kv_hbm.at[dest % 2, half, pair], kv_l.at[kv_piece(me, half), pair],
                      kv_send.at[g, dest, half], kv_recv.at[g, me, half], dest)

    def kv_own(g, half):
        pair = pl.ds(g * 2, 2)
        return pltpu.make_async_copy(kv_hbm.at[core, half, pair], kv_l.at[kv_piece(me, half), pair], kv_loc.at[g, half])

    def kv_arrive(g, source, half):
        pair = pl.ds(g * 2, 2)
        return remote(kv_hbm.at[core, half, pair], kv_l.at[kv_piece(source, half), pair],
                      kv_send.at[g, source, half], kv_recv.at[g, source, half], source)

    def kv_issue(g):
        for half in range(2):
            kv_own(g, half).start()
        for step in range(1, CP):
            dest = (me + step) % CP
            kv_copy(g, dest, 0).start()

            @pl.when(dest // 2 <= chip)
            def _():
                kv_copy(g, dest, 1).start()

    def kv_wait(g):
        for half in range(2):
            kv_own(g, half).wait()
        for step in range(1, CP):
            source = (me + step) % CP
            kv_arrive(g, source, 0).wait_recv()

            @pl.when(chip <= source // 2)
            def _():
                kv_arrive(g, source, 1).wait_recv()

    def kv_drain(g):
        for step in range(1, CP):
            dest = (me + step) % CP
            kv_copy(g, dest, 0).wait_send()

            @pl.when(dest // 2 <= chip)
            def _():
                kv_copy(g, dest, 1).wait_send()

    def q_views(g, half, slot, head):
        pair = pl.ds(g * 2, 2)
        ring = g % Q_RING
        return ((q_hbm.at[pair, half, :, head], q_l.at[ring, slot]),
                (g_hbm.at[pair, half, :, head], g_l.at[ring, slot]),
                (cs_hbm.at[half, pair], cs_l.at[slot, pl.ds(g % (CS_RING // 2) * 2, 2)]))

    def q_local(g):
        return [pltpu.make_async_copy(src, dst, q_loc.at[g, i, half]) for half in range(2)
                for i, (src, dst) in enumerate(q_views(g, half, own_slot(half), core))]

    def q_out(g):
        return [remote(src, dst, q_send.at[g, i, half], q_recv.at[g, i, half], sibling) for half in range(2)
                for i, (src, dst) in enumerate(q_views(g, half, own_slot(half), 1 - core))]

    def q_arriving(g):
        return [remote(src, dst, q_send.at[g, i, half], q_recv.at[g, i, half], sibling) for half in range(2)
                for i, (src, dst) in enumerate(q_views(g, half, sib_slot(half), core))]

    def q_issue(g):
        for copy in q_local(g) + q_out(g):
            copy.start()

    def q_wait(g):
        for copy in q_local(g):
            copy.wait()
        for copy in q_arriving(g):
            copy.wait_recv()

    def o_local(b):
        return [pltpu.make_async_copy(o_st.at[b % 2, a, own_slot(half)], ref.at[b, half, :, core],
                                      o_loc.at[b % 2, a, half])
                for a, ref in enumerate((out_hbm, dq_hbm)) for half in range(2)]

    def o_out(b):
        return [remote(o_st.at[b % 2, a, sib_slot(half)], ref.at[b, half, :, core],
                       o_send.at[b % 2, a, half], o_recv.at[b, a, half], sibling)
                for a, ref in enumerate((out_hbm, dq_hbm)) for half in range(2)]

    def o_drain(b):
        for copy in o_local(b):
            copy.wait()
        for copy in o_out(b):
            copy.wait_send()

    def o_wait(b):
        for a, ref in enumerate((out_hbm, dq_hbm)):
            for half in range(2):
                remote(o_st.at[b % 2, a, own_slot(half)], ref.at[b, half, :, 1 - core],
                       o_send.at[b % 2, a, half], o_recv.at[b, a, half], sibling).wait_recv()

    def f_local(b):
        return [pltpu.make_async_copy(f_st.at[b % 2, a, own_slot(half)], ref.at[core, b, half], f_loc.at[b % 2, a, half])
                for a, ref in enumerate((dk_hbm, dv_hbm)) for half in range(2)]

    def f_out(b):
        return [remote(f_st.at[b % 2, a, sib_slot(half)], ref.at[core, b, half],
                       f_send.at[b % 2, a, half], f_recv.at[b, a, half], sibling)
                for a, ref in enumerate((dk_hbm, dv_hbm)) for half in range(2)]

    def f_drain(b):
        for copy in f_local(b):
            copy.wait()
        for copy in f_out(b):
            copy.wait_send()

    def f_wait(b):
        for a, ref in enumerate((dk_hbm, dv_hbm)):
            for half in range(2):
                remote(f_st.at[b % 2, a, own_slot(half)], ref.at[1 - core, b, half],
                       f_send.at[b % 2, a, half], f_recv.at[b, a, half], sibling).wait_recv()

    def s1_copy(b, m):
        first, _ = partners(b)
        target = first if m < 2 else diag
        block = target if m % 2 == 0 else 7 - target
        return remote(part.at[b % PARTS, :, block], s1_l.at[b % S1_RING, m], s1_send.at[b % PARTS, m], s1_recv.at[b, m],
                      first * 2 + core)

    def s1_each(b, do):
        first, _ = partners(b)
        for m in range(4):
            if m % 2 == 0:
                do(s1_copy(b, m))
            else:
                target = first if m < 2 else diag

                @pl.when(target > chip)
                def _():
                    do(s1_copy(b, m))

    def s2_copy(b, m):
        _, second = partners(b)
        return remote(s1_l.at[b % S1_RING, 2 + m], s2_l.at[b % S2_RING, m], s2_send.at[b, m], s2_recv.at[b, m], second * 2 + core)

    def s2_send_high(b):
        first, second = partners(b)
        return jnp.logical_or(second > chip, second > first)

    def s2_recv_high(b):
        _, second = partners(b)
        return jnp.logical_or(chip > second, chip > diag)

    def s2_each(b, do):
        do(s2_copy(b, 0))

        @pl.when(s2_send_high(b))
        def _():
            do(s2_copy(b, 1))

    def add_step(b):
        first, second = partners(b)
        ring = b % PARTS
        s1_copy(b, 0).wait_recv()
        s1_copy(b, 2).wait_recv()

        @pl.when(chip > first)
        def _():
            s1_copy(b, 1).wait_recv()

        @pl.when(second > first)
        def _():
            s1_copy(b, 3).wait_recv()

        at = b % S1_RING
        for i in range(2):
            s1_l[at, 0, i] = s1_l[at, 0, i] + part[ring, i, chip]
            s1_l[at, 2, i] = s1_l[at, 2, i] + part[ring, i, second]
            s1_l[at, 1, i] = jnp.where(chip > first, s1_l[at, 1, i], 0.0) + part[ring, i, 7 - chip]
            s1_l[at, 3, i] = jnp.where(second > first, s1_l[at, 3, i], 0.0) + part[ring, i, 7 - second]

    def end_step(b):
        s2_copy(b, 0).wait_recv()
        has_high = s2_recv_high(b)

        @pl.when(has_high)
        def _():
            s2_copy(b, 1).wait_recv()

        @pl.when(b >= 2)
        def _():
            f_drain(b - 2)

        s2_each(b, lambda copy: copy.wait_send())
        ring = b % 2
        for m in range(2):
            for i in range(2):
                other = s2_l[b % S2_RING, m, i]
                if m == 1:
                    other = jnp.where(has_high, other, 0.0)
                total = (s1_l[b % S1_RING, m, i] + other).T
                for sub in range(2):
                    slot = m * 2 + sub
                    x = total[sub * PIECE:(sub + 1) * PIECE]
                    if i == 0:
                        x = x * cs_l[slot, b % CS_RING, 0] - swap_pairs(x) * cs_l[slot, b % CS_RING, 1]
                    f_st[ring, i, slot] = x.astype(jnp.bfloat16)

    def compute(b):
        ring, g_ring, b_in, c_ring = b % PARTS, (b // 2) % Q_RING, b % 2, b % CS_RING

        @pl.when(b >= PARTS)
        def _():
            s1_each(b - PARTS, lambda copy: copy.wait_send())

        @pl.when(b >= 2)
        def _():
            o_drain(b - 2)

        for piece in range(2 * CP):
            k_p, v_p = kv_l[piece, b, 0], kv_l[piece, b, 1]
            if piece >= CP:
                needed = (2 * CP - 1 - piece) // 2 >= chip
                k_p, v_p = jnp.where(needed, k_p, 0), jnp.where(needed, v_p, 0)
            k_s[piece * PIECE:(piece + 1) * PIECE, :] = k_p.astype(jnp.bfloat16)
            v_s[piece * PIECE:(piece + 1) * PIECE, :] = v_p.astype(jnp.bfloat16)
        for i in range(2):
            for j in range(8):
                part[ring, i, j] = jnp.zeros((DIM, DIM), jnp.float32)

        def tile(slot, n_keys, q_start):
            rows = PIECE * GROUP
            cos = jnp.broadcast_to(cs_l[slot, c_ring, 0][:, None, :], (PIECE, GROUP, DIM)).reshape(rows, DIM)
            sin = jnp.broadcast_to(cs_l[slot, c_ring, 1][:, None, :], (PIECE, GROUP, DIM)).reshape(rows, DIM)
            qx = q_l[g_ring, slot, b_in].astype(jnp.float32).reshape(rows, DIM)
            qr = (qx * cos + swap_pairs(qx) * sin).astype(jnp.bfloat16)
            gr = g_l[g_ring, slot, b_in].astype(jnp.float32).reshape(rows, DIM).astype(jnp.bfloat16)
            out, dq, dk_t, dv_t = attend_tile(qr, gr, k_s, v_s, n_keys, q_start, scale)
            dq = dq * cos - swap_pairs(dq) * sin
            o_st[b % 2, 0, slot] = out.reshape(PIECE, GROUP, DIM).astype(jnp.bfloat16)
            o_st[b % 2, 1, slot] = dq.reshape(PIECE, GROUP, DIM).astype(jnp.bfloat16)
            for j in range(n_keys // DIM):
                part[ring, 0, j] += dk_t[:, j * DIM:(j + 1) * DIM]
                part[ring, 1, j] += dv_t[:, j * DIM:(j + 1) * DIM]

        def variant(n_low, n_high):
            def high(i, carry):
                tile(2 + i, n_high, (2 * CP - 2 - 2 * chip + i) * PIECE)
                return carry

            def low(i, carry):
                tile(i, n_low, (2 * chip + i) * PIECE)
                return carry

            lax.fori_loop(0, 2, high, 0)
            lax.fori_loop(0, 2, low, 0)

        @pl.when(chip < 2)
        def _():
            variant(CP * PIECE // 2, 2 * CP * PIECE)

        @pl.when(chip >= 2)
        def _():
            variant(CP * PIECE, CP * PIECE * 3 // 2)

    barrier = pltpu.get_barrier_semaphore()
    for step in range(1, CP):
        pl.semaphore_signal(barrier, inc=1, device_id={'cp': (me + step) % CP}, device_id_type=MESH)
    pl.semaphore_wait(barrier, CP - 1)

    ahead = jnp.maximum(2, 4 - chip)
    for g in range(4):
        if g < 2:
            kv_issue(g)
        else:
            @pl.when(g < ahead)
            def _(g=g):
                kv_issue(g)
        if g == 0:
            q_issue(0)

    def step(it, carry):
        even = it % 2 == 0

        @pl.when(jnp.logical_and(even, jnp.logical_and(it >= 4, it + 2 < n_batch)))
        def _():
            o_wait(it - 4)
            o_wait(it - 3)

        @pl.when(jnp.logical_and(even, it + 2 < n_batch))
        def _():
            q_issue(it // 2 + 1)

        @pl.when(jnp.logical_and(even, it // 2 + ahead < n_groups))
        def _():
            kv_issue(it // 2 + ahead)

        @pl.when(jnp.logical_and(it >= LAG_ADD, it < n_batch + LAG_ADD))
        def _():
            add_step(it - LAG_ADD)

        @pl.when(it >= LAG_END)
        def _():
            end_step(it - LAG_END)

        @pl.when(jnp.logical_and(it >= LAG_ADD, it < n_batch + LAG_ADD))
        def _():
            s2_each(it - LAG_ADD, lambda copy: copy.start())

        @pl.when(jnp.logical_and(even, it < n_batch))
        def _():
            kv_wait(it // 2)
            q_wait(it // 2)

        @pl.when(it < n_batch)
        def _():
            compute(it)
            s1_each(it, lambda copy: copy.start())
            for copy in o_local(it) + o_out(it):
                copy.start()

        @pl.when(it >= LAG_END)
        def _():
            for copy in f_local(it - LAG_END) + f_out(it - LAG_END):
                copy.start()

        return carry

    lax.fori_loop(0, n_batch + LAG_END, step, 0)

    for b in range(n_batch - PARTS, n_batch):
        s1_each(b, lambda copy: copy.wait_send())
    for b in range(n_batch - 2, n_batch):
        o_drain(b)
        f_drain(b)

    def drain_group(g, carry):
        kv_drain(g)
        for copy in q_out(g):
            copy.wait_send()
        return carry

    def drain_batch(b, carry):
        f_wait(b)
        return carry

    def drain_out(b, carry):
        o_wait(b)
        return carry

    lax.fori_loop(0, n_groups, drain_group, 0)
    lax.fori_loop(0, n_batch, drain_batch, 0)
    lax.fori_loop(n_batch - 6, n_batch, drain_out, 0)


def fused_attention(query, grad_out, tables, kv):
    n_batch = query.shape[0]
    n_groups = n_batch // 2
    sem = pltpu.SemaphoreType.DMA
    f32, bf16 = jnp.float32, jnp.bfloat16
    any_spec = pl.BlockSpec(memory_space=pl.ANY)
    return pl.pallas_call(
        functools.partial(fused_kernel, n_batch),
        out_shape=(jax.ShapeDtypeStruct(query.shape, bf16), jax.ShapeDtypeStruct(query.shape, bf16),
                   jax.ShapeDtypeStruct((2, n_batch, 2, PIECE, DIM), bf16),
                   jax.ShapeDtypeStruct((2, n_batch, 2, PIECE, DIM), bf16)),
        in_specs=[any_spec] * 4,
        out_specs=(any_spec,) * 4,
        scratch_shapes=[
            pltpu.VMEM((Q_RING, 4, 2, PIECE, GROUP, DIM), bf16),
            pltpu.VMEM((Q_RING, 4, 2, PIECE, GROUP, DIM), bf16),
            pltpu.VMEM((4, CS_RING, 2, PIECE, DIM), f32),
            pltpu.VMEM((2 * CP, n_batch, 2, PIECE, DIM), bf16),
            pltpu.VMEM((S1_RING, 4, 2, DIM, DIM), f32),
            pltpu.VMEM((S2_RING, 2, 2, DIM, DIM), f32),
            pltpu.VMEM((PARTS, 2, 8, DIM, DIM), f32),
            pltpu.VMEM((2, 2, 4, PIECE, GROUP, DIM), bf16),
            pltpu.VMEM((2, 2, 4, PIECE, DIM), bf16),
            pltpu.VMEM((2 * CP * PIECE, DIM), bf16),
            pltpu.VMEM((2 * CP * PIECE, DIM), bf16),
            sem((n_groups, 2)), sem((n_groups, CP, 2)), sem((n_groups, CP, 2)),
            sem((n_groups, 3, 2)), sem((n_groups, 3, 2)), sem((n_groups, 3, 2)),
            sem((PARTS, 4)), sem((n_batch, 4)), sem((n_batch, 2)), sem((n_batch, 2)),
            sem((2, 2, 2)), sem((2, 2, 2)), sem((n_batch, 2, 2)),
            sem((2, 2, 2)), sem((2, 2, 2)), sem((n_batch, 2, 2)),
        ],
        compiler_params=pltpu.CompilerParams(collective_id=0, has_side_effects=True, vmem_limit_bytes=VMEM_MIB * 2 ** 20),
    )(query, grad_out, tables, kv)


def hand_on_kernel(a_ref, b_ref, c_ref, d_ref, sems):
    copies = [pltpu.make_async_copy(a_ref, c_ref, sems.at[0]), pltpu.make_async_copy(b_ref, d_ref, sems.at[1])]
    for copy in copies:
        copy.start()
    for copy in copies:
        copy.wait()


def hand_on(a, b):
    any_spec = pl.BlockSpec(memory_space=pl.ANY)
    return pl.pallas_call(hand_on_kernel, in_specs=[any_spec] * 2, out_specs=(any_spec,) * 2,
                          out_shape=(jax.ShapeDtypeStruct(a.shape, a.dtype), jax.ShapeDtypeStruct(b.shape, b.dtype)),
                          scratch_shapes=[pltpu.SemaphoreType.DMA((2,))],
                          compiler_params=pltpu.CompilerParams(vmem_limit_bytes=2 ** 20))(a, b)


def cos_sin(angles):
    turns = jnp.floor(angles * (2.0 / math.pi) + 0.5)
    rest = ((angles - turns * 1.5703125) - turns * 4.837512969970703125e-4) - turns * 7.549789948768648e-8
    sq = rest * rest
    sine = ((-1.9515295891e-4 * sq + 8.3321608736e-3) * sq - 1.6666654611e-1) * sq * rest + rest
    cosine = ((2.443315711809948e-5 * sq - 1.388731625493765e-3) * sq + 4.166664568298827e-2) * sq * sq - 0.5 * sq + 1.0
    quarter = turns.astype(jnp.int32) % 4
    odd = quarter % 2 == 1
    cos_v = jnp.where(odd, sine, cosine)
    sin_v = jnp.where(odd, cosine, sine)
    cos_v = jnp.where((quarter == 1) | (quarter == 2), -cos_v, cos_v)
    sin_v = jnp.where(quarter >= 2, -sin_v, sin_v)
    return cos_v, sin_v


def solution(mesh):
    head_spec = P(None, 'cp', 'tp', None)
    pos_spec = P(None, 'cp')

    def local_step(query, keys, values, positions, grad_out):
        batch, length, n_heads, dim = query.shape
        lanes = jnp.arange(dim, dtype=jnp.int32)
        freq_expo = (lanes // 2).astype(jnp.float32) * (2.0 / dim)
        inv_freq = 1.0 / (ROPE_THETA ** freq_expo)
        angles = positions.astype(jnp.float32)[:, :, None] * inv_freq
        cos_t, sin_t = cos_sin(angles)
        sin_t = sin_t * jnp.where(lanes % 2 == 0, -1.0, 1.0)
        swap_mat = (lanes[:, None] == (lanes ^ 1)[None, :]).astype(jnp.bfloat16)
        k_t = keys.transpose(2, 0, 1, 3)
        k_swap = jnp.einsum('hbtd,de->hbte', k_t, swap_mat, preferred_element_type=jnp.float32)
        k_rot = (k_t.astype(jnp.float32) * cos_t + k_swap * sin_t).astype(jnp.bfloat16)
        by_half = (2, batch, 2, PIECE, dim)
        kv = jnp.stack([k_rot.reshape(by_half), values.transpose(2, 0, 1, 3).reshape(by_half)], axis=3)
        kv = kv.transpose(0, 2, 1, 3, 4, 5)
        tables = jnp.stack([cos_t.reshape(by_half[1:]), sin_t.reshape(by_half[1:])], axis=2).transpose(1, 0, 2, 3, 4)
        split = (batch, 2, PIECE, 2, GROUP, dim)
        out, dq, dk, dv = fused_attention(query.reshape(split), grad_out.reshape(split), tables, kv)
        out, dq = hand_on(out, dq)
        back = (2, batch, length, dim)
        return out.reshape(query.shape), dq.reshape(query.shape), dk.reshape(back).transpose(1, 2, 0, 3), dv.reshape(back).transpose(1, 2, 0, 3)

    return jax.shard_map(local_step, mesh=mesh,
                         in_specs=(head_spec, head_spec, head_spec, pos_spec, head_spec),
                         out_specs=(head_spec, head_spec, head_spec, head_spec), check_vma=False)
```

```python
import functools
import math

import jax
import jax.numpy as jnp
from jax import lax
from jax.experimental import pallas as pl
from jax.experimental.pallas import tpu as pltpu
from jax.sharding import PartitionSpec as P

ROPE_THETA = 1000000.0
LOG2E = 1.4426950408889634
MESH = pl.DeviceIdType.MESH
CP = 8
PIECE = 64
GROUP = 8
DIM = 128
PARTS = 4
LAG_ADD = 3
LAG_END = 5
KEY_BLOCK = 256
VMEM_MIB = 36
Q_RING = 3
CS_RING = 12
S1_RING = 10
S2_RING = 6


def swap_pairs(x):
    lane = lax.broadcasted_iota(jnp.int32, x.shape, 1)
    return jnp.where(lane % 2 == 0, pltpu.roll(x, 127, 1), pltpu.roll(x, 1, 1))


def dot_nt(a, b):
    return lax.dot_general(a, b, (((1,), (1,)), ((), ())), preferred_element_type=jnp.float32)


def dot_nn(a, b):
    return lax.dot_general(a, b, (((1,), (0,)), ((), ())), preferred_element_type=jnp.float32)


def attend_tile(qr, gr, k_view, v_view, n_keys, q_start, scale):
    n_blk = n_keys // KEY_BLOCK
    scores = []
    for j in range(n_blk):
        s = dot_nt(qr, k_view[j * KEY_BLOCK:(j + 1) * KEY_BLOCK, :])
        if j == n_blk - 1:
            q_idx = q_start + lax.broadcasted_iota(jnp.int32, s.shape, 0) // GROUP
            k_idx = j * KEY_BLOCK + lax.broadcasted_iota(jnp.int32, s.shape, 1)
            s = jnp.where(k_idx <= q_idx, s, -jnp.inf)
        scores.append(s)
    row_max = jnp.max(functools.reduce(jnp.maximum, scores), axis=1, keepdims=True)
    expo = [jnp.exp2((s - row_max) * (scale * LOG2E)) for s in scores]
    row_sum = jnp.sum(functools.reduce(jnp.add, expo), axis=1, keepdims=True)
    inv = 1.0 / row_sum
    probs = [e * inv for e in expo]
    p_all = jnp.concatenate([p.astype(jnp.bfloat16) for p in probs], axis=1)
    out = dot_nn(p_all, v_view[0:n_keys, :])
    delta = jnp.sum(out * gr.astype(jnp.float32), axis=1, keepdims=True)
    ds = []
    for j in range(n_blk):
        dp = dot_nt(gr, v_view[j * KEY_BLOCK:(j + 1) * KEY_BLOCK, :])
        ds.append((probs[j] * (dp - delta)).astype(jnp.bfloat16))
    ds_all = jnp.concatenate(ds, axis=1)
    dq = dot_nn(ds_all, k_view[0:n_keys, :]) * scale
    dv_t = dot_nn(gr.T, p_all)
    dk_t = dot_nn(qr.T, ds_all) * scale
    return out, dq, dk_t, dv_t


def fused_kernel(n_batch, q_hbm, g_hbm, cos_hbm, sin_hbm, kv_hbm, out_hbm, dq_hbm, dk_hbm, dv_hbm,
                 q_l, g_l, cs_l, kv_l, s1_l, s2_l, part, o_st, f_st, k_s, v_s,
                 kv_loc, kv_send, kv_recv, pass_send, q_loc, q_send, q_recv, s1_send, s1_recv, s2_send, s2_recv,
                 o_loc, o_send, o_recv, f_loc, f_send, f_recv):
    me = lax.axis_index('cp')
    chip, core = me // 2, me % 2
    sibling = chip * 2 + 1 - core
    n_groups = n_batch // 2
    scale = DIM ** -0.5
    diag = 3 - chip

    def own_slot(half):
        return core if half == 0 else 3 - core

    def sib_slot(half):
        return 1 - core if half == 0 else 2 + core

    def partners(b):
        along_x = chip + 1 - 2 * (chip % 2)
        along_y = (chip + 2) % 4
        odd = b % 2
        return along_x * (1 - odd) + along_y * odd, along_y * (1 - odd) + along_x * odd

    def remote(src, dst, send, recv, device):
        return pltpu.make_async_remote_copy(src_ref=src, dst_ref=dst, send_sem=send, recv_sem=recv,
                                            device_id={'cp': device}, device_id_type=MESH)

    def kv_piece(device, half):
        return device if half == 0 else 2 * CP - 1 - device

    def kv_copy(g, dest, half):
        pair = pl.ds(g * 2, 2)
        return remote(kv_hbm.at[dest % 2, half, pair], kv_l.at[kv_piece(me, half), pair],
                      kv_send.at[g, dest, half], kv_recv.at[g, me, half], dest)

    def kv_own(g, half):
        pair = pl.ds(g * 2, 2)
        return pltpu.make_async_copy(kv_hbm.at[core, half, pair], kv_l.at[kv_piece(me, half), pair], kv_loc.at[g, half])

    near_x = chip + 1 - 2 * (chip % 2)
    near_y = (chip + 2) % 4
    near = (sibling, near_x * 2, near_x * 2 + 1, near_y * 2, near_y * 2 + 1)
    far = (diag * 2, diag * 2 + 1)

    def kv_arrive(g, source, half):
        pair = pl.ds(g * 2, 2)
        return remote(kv_hbm.at[core, half, pair], kv_l.at[kv_piece(source, half), pair],
                      kv_send.at[g, source, half], kv_recv.at[g, source, half], source)

    def kv_each(g, do):
        for dest in near:
            do(kv_copy(g, dest, 0))

            @pl.when(dest // 2 <= chip)
            def _(dest=dest):
                do(kv_copy(g, dest, 1))

        @pl.when(chip == 2)
        def _():
            for dest in far:
                do(kv_copy(g, dest, 1))

    def kv_issue(g):
        for half in range(2):
            kv_own(g, half).start()
        kv_each(g, lambda copy: copy.start())

    def kv_wait_from(g, sources):
        for source in sources:
            kv_arrive(g, source, 0).wait_recv()

            @pl.when(chip <= source // 2)
            def _(source=source):
                kv_arrive(g, source, 1).wait_recv()

    def kv_pass(g, i, source_chip, source_core, half):
        pair = pl.ds(g * 2, 2)
        source = source_chip * 2 + source_core
        place = kv_l.at[kv_piece(source, half), pair]
        return remote(place, place, pass_send.at[g, i, source_core, half], kv_recv.at[g, source, half],
                      (3 - source_chip) * 2 + core)

    def kv_pass_each(g, do):
        from_last = (g + chip + 1) % 2

        @pl.when(jnp.logical_or(chip == 1, chip == 2))
        def _():
            for source_core in range(2):
                do(kv_pass(g, 0, 3 * from_last, source_core, 0))

                @pl.when(from_last == 1)
                def _(source_core=source_core):
                    do(kv_pass(g, 0, 3 * from_last, source_core, 1))

        @pl.when(chip == 3)
        def _():
            for i in range(2):
                for source_core in range(2):
                    do(kv_pass(g, i, 1 + i, source_core, 0))

    def kv_near(g):
        kv_wait_from(g, near)
        kv_pass_each(g, lambda copy: copy.start())

    def kv_far(g):
        for half in range(2):
            kv_own(g, half).wait()
        kv_wait_from(g, far)

    def kv_drain(g):
        kv_each(g, lambda copy: copy.wait_send())
        kv_pass_each(g, lambda copy: copy.wait_send())

    def q_views(g, half, slot, head):
        pair = pl.ds(g * 2, 2)
        ring = g % Q_RING
        held = pl.ds(g % (CS_RING // 2) * 2, 2)
        return ((q_hbm.at[pair, half, :, head], q_l.at[ring, slot]),
                (g_hbm.at[pair, half, :, head], g_l.at[ring, slot]),
                (cos_hbm.at[pair, half], cs_l.at[slot, held, 0]),
                (sin_hbm.at[pair, half], cs_l.at[slot, held, 1]))

    def q_local(g):
        return [pltpu.make_async_copy(src, dst, q_loc.at[g, i, half]) for half in range(2)
                for i, (src, dst) in enumerate(q_views(g, half, own_slot(half), core))]

    def q_out(g):
        return [remote(src, dst, q_send.at[g, i, half], q_recv.at[g, i, half], sibling) for half in range(2)
                for i, (src, dst) in enumerate(q_views(g, half, own_slot(half), 1 - core))]

    def q_arriving(g):
        return [remote(src, dst, q_send.at[g, i, half], q_recv.at[g, i, half], sibling) for half in range(2)
                for i, (src, dst) in enumerate(q_views(g, half, sib_slot(half), core))]

    def q_issue(g):
        for copy in q_local(g) + q_out(g):
            copy.start()

    def q_wait(g):
        for copy in q_local(g):
            copy.wait()
        for copy in q_arriving(g):
            copy.wait_recv()

    def o_local(b):
        return [pltpu.make_async_copy(o_st.at[b % 2, a, own_slot(half)], ref.at[b, half, :, core],
                                      o_loc.at[b % 2, a, half])
                for a, ref in enumerate((out_hbm, dq_hbm)) for half in range(2)]

    def o_out(b):
        return [remote(o_st.at[b % 2, a, sib_slot(half)], ref.at[b, half, :, core],
                       o_send.at[b % 2, a, half], o_recv.at[b, a, half], sibling)
                for a, ref in enumerate((out_hbm, dq_hbm)) for half in range(2)]

    def o_drain(b):
        for copy in o_local(b):
            copy.wait()
        for copy in o_out(b):
            copy.wait_send()

    def o_wait(b):
        for a, ref in enumerate((out_hbm, dq_hbm)):
            for half in range(2):
                remote(o_st.at[b % 2, a, own_slot(half)], ref.at[b, half, :, 1 - core],
                       o_send.at[b % 2, a, half], o_recv.at[b, a, half], sibling).wait_recv()

    def f_local(b):
        return [pltpu.make_async_copy(f_st.at[b % 2, a, own_slot(half)], ref.at[core, b, half], f_loc.at[b % 2, a, half])
                for a, ref in enumerate((dk_hbm, dv_hbm)) for half in range(2)]

    def f_out(b):
        return [remote(f_st.at[b % 2, a, sib_slot(half)], ref.at[core, b, half],
                       f_send.at[b % 2, a, half], f_recv.at[b, a, half], sibling)
                for a, ref in enumerate((dk_hbm, dv_hbm)) for half in range(2)]

    def f_drain(b):
        for copy in f_local(b):
            copy.wait()
        for copy in f_out(b):
            copy.wait_send()

    def f_wait(b):
        for a, ref in enumerate((dk_hbm, dv_hbm)):
            for half in range(2):
                remote(f_st.at[b % 2, a, own_slot(half)], ref.at[1 - core, b, half],
                       f_send.at[b % 2, a, half], f_recv.at[b, a, half], sibling).wait_recv()

    def s1_copy(b, m):
        first, _ = partners(b)
        target = first if m < 2 else diag
        block = target if m % 2 == 0 else 7 - target
        return remote(part.at[b % PARTS, :, block], s1_l.at[b % S1_RING, m], s1_send.at[b % PARTS, m], s1_recv.at[b, m],
                      first * 2 + core)

    def s1_high(b, do):
        first, _ = partners(b)
        for m, target in ((1, first), (3, diag)):
            @pl.when(target > chip)
            def _(m=m):
                do(s1_copy(b, m))

    def s1_low(b, do):
        for m in (0, 2):
            do(s1_copy(b, m))

    def s1_each(b, do):
        s1_high(b, do)
        s1_low(b, do)

    def s2_copy(b, m):
        _, second = partners(b)
        return remote(s1_l.at[b % S1_RING, 2 + m], s2_l.at[b % S2_RING, m], s2_send.at[b, m], s2_recv.at[b, m], second * 2 + core)

    def s2_send_high(b):
        first, second = partners(b)
        return jnp.logical_or(second > chip, second > first)

    def s2_recv_high(b):
        _, second = partners(b)
        return jnp.logical_or(chip > second, chip > diag)

    def s2_each(b, do):
        do(s2_copy(b, 0))

        @pl.when(s2_send_high(b))
        def _():
            do(s2_copy(b, 1))

    def add_step(b):
        first, second = partners(b)
        ring = b % PARTS
        s1_copy(b, 0).wait_recv()
        s1_copy(b, 2).wait_recv()

        @pl.when(chip > first)
        def _():
            s1_copy(b, 1).wait_recv()

        @pl.when(second > first)
        def _():
            s1_copy(b, 3).wait_recv()

        at = b % S1_RING
        for i in range(2):
            s1_l[at, 0, i] = s1_l[at, 0, i] + part[ring, i, chip]
            s1_l[at, 2, i] = s1_l[at, 2, i] + part[ring, i, second]
            s1_l[at, 1, i] = jnp.where(chip > first, s1_l[at, 1, i], 0.0) + part[ring, i, 7 - chip]
            s1_l[at, 3, i] = jnp.where(second > first, s1_l[at, 3, i], 0.0) + part[ring, i, 7 - second]

    def end_step(b):
        s2_copy(b, 0).wait_recv()
        has_high = s2_recv_high(b)

        @pl.when(has_high)
        def _():
            s2_copy(b, 1).wait_recv()

        @pl.when(b >= 2)
        def _():
            f_drain(b - 2)

        s2_each(b, lambda copy: copy.wait_send())
        ring = b % 2
        for m in range(2):
            for i in range(2):
                other = s2_l[b % S2_RING, m, i]
                if m == 1:
                    other = jnp.where(has_high, other, 0.0)
                total = (s1_l[b % S1_RING, m, i] + other).T
                for sub in range(2):
                    slot = m * 2 + sub
                    x = total[sub * PIECE:(sub + 1) * PIECE]
                    if i == 0:
                        x = x * cs_l[slot, b % CS_RING, 0] - swap_pairs(x) * cs_l[slot, b % CS_RING, 1]
                    f_st[ring, i, slot] = x.astype(jnp.bfloat16)

    def compute(b):
        ring, g_ring, b_in, c_ring = b % PARTS, (b // 2) % Q_RING, b % 2, b % CS_RING

        @pl.when(b >= PARTS)
        def _():
            s1_each(b - PARTS, lambda copy: copy.wait_send())

        @pl.when(b >= 2)
        def _():
            o_drain(b - 2)

        for piece in range(2 * CP):
            k_p, v_p = kv_l[piece, b, 0], kv_l[piece, b, 1]
            if piece >= CP:
                needed = (2 * CP - 1 - piece) // 2 >= chip
                k_p, v_p = jnp.where(needed, k_p, 0), jnp.where(needed, v_p, 0)
            k_s[piece * PIECE:(piece + 1) * PIECE, :] = k_p.astype(jnp.bfloat16)
            v_s[piece * PIECE:(piece + 1) * PIECE, :] = v_p.astype(jnp.bfloat16)
        for i in range(2):
            for j in range(8):
                part[ring, i, j] = jnp.zeros((DIM, DIM), jnp.float32)

        def tile(slot, n_keys, q_start):
            rows = PIECE * GROUP
            cos = jnp.broadcast_to(cs_l[slot, c_ring, 0][:, None, :], (PIECE, GROUP, DIM)).reshape(rows, DIM)
            sin = jnp.broadcast_to(cs_l[slot, c_ring, 1][:, None, :], (PIECE, GROUP, DIM)).reshape(rows, DIM)
            qx = q_l[g_ring, slot, b_in].astype(jnp.float32).reshape(rows, DIM)
            qr = (qx * cos + swap_pairs(qx) * sin).astype(jnp.bfloat16)
            gr = g_l[g_ring, slot, b_in].astype(jnp.float32).reshape(rows, DIM).astype(jnp.bfloat16)
            out, dq, dk_t, dv_t = attend_tile(qr, gr, k_s, v_s, n_keys, q_start, scale)
            dq = dq * cos - swap_pairs(dq) * sin
            o_st[b % 2, 0, slot] = out.reshape(PIECE, GROUP, DIM).astype(jnp.bfloat16)
            o_st[b % 2, 1, slot] = dq.reshape(PIECE, GROUP, DIM).astype(jnp.bfloat16)
            for j in reversed(range(n_keys // DIM)):
                part[ring, 0, j] += dk_t[:, j * DIM:(j + 1) * DIM]
                part[ring, 1, j] += dv_t[:, j * DIM:(j + 1) * DIM]

        def high(n_keys):
            def body(i, carry):
                tile(2 + i, n_keys, (2 * CP - 2 - 2 * chip + i) * PIECE)
                return carry

            lax.fori_loop(0, 2, body, 0)

        def low(n_keys):
            def body(i, carry):
                tile(i, n_keys, (2 * chip + i) * PIECE)
                return carry

            lax.fori_loop(0, 2, body, 0)

        @pl.when(chip < 2)
        def _():
            high(2 * CP * PIECE)

        @pl.when(chip >= 2)
        def _():
            high(CP * PIECE * 3 // 2)

        s1_high(b, lambda copy: copy.start())

        @pl.when(chip < 2)
        def _():
            low(CP * PIECE // 2)

        @pl.when(chip >= 2)
        def _():
            low(CP * PIECE)

    barrier = pltpu.get_barrier_semaphore()
    for step in range(1, CP):
        pl.semaphore_signal(barrier, inc=1, device_id={'cp': (me + step) % CP}, device_id_type=MESH)
    pl.semaphore_wait(barrier, CP - 1)

    kv_issue(0)
    q_issue(0)
    kv_issue(1)
    kv_near(0)

    def step(it, carry):
        even = it % 2 == 0

        @pl.when(jnp.logical_and(even, jnp.logical_and(it >= 4, it + 2 < n_batch)))
        def _():
            o_wait(it - 4)
            o_wait(it - 3)

        @pl.when(jnp.logical_and(even, it + 2 < n_batch))
        def _():
            q_issue(it // 2 + 1)

        @pl.when(jnp.logical_and(even, it // 2 + 2 < n_groups))
        def _():
            kv_issue(it // 2 + 2)

        @pl.when(jnp.logical_and(it >= LAG_ADD, it < n_batch + LAG_ADD))
        def _():
            add_step(it - LAG_ADD)

        @pl.when(it >= LAG_END)
        def _():
            end_step(it - LAG_END)

        @pl.when(jnp.logical_and(it >= LAG_ADD, it < n_batch + LAG_ADD))
        def _():
            s2_each(it - LAG_ADD, lambda copy: copy.start())

        @pl.when(jnp.logical_and(even, it // 2 + 1 < n_groups))
        def _():
            kv_near(it // 2 + 1)

        @pl.when(jnp.logical_and(even, it < n_batch))
        def _():
            kv_far(it // 2)
            q_wait(it // 2)

        @pl.when(it < n_batch)
        def _():
            compute(it)
            s1_low(it, lambda copy: copy.start())
            for copy in o_local(it) + o_out(it):
                copy.start()

        @pl.when(it >= LAG_END)
        def _():
            for copy in f_local(it - LAG_END) + f_out(it - LAG_END):
                copy.start()

        return carry

    lax.fori_loop(0, n_batch + LAG_END, step, 0)

    for b in range(n_batch - PARTS, n_batch):
        s1_each(b, lambda copy: copy.wait_send())
    for b in range(n_batch - 2, n_batch):
        o_drain(b)
        f_drain(b)

    def drain_group(g, carry):
        kv_drain(g)
        for copy in q_out(g):
            copy.wait_send()
        return carry

    def drain_batch(b, carry):
        f_wait(b)
        return carry

    def drain_out(b, carry):
        o_wait(b)
        return carry

    lax.fori_loop(0, n_groups, drain_group, 0)
    lax.fori_loop(0, n_batch, drain_batch, 0)
    lax.fori_loop(n_batch - 6, n_batch, drain_out, 0)


def fused_attention(query, grad_out, cos_t, sin_t, kv):
    n_batch = query.shape[0]
    n_groups = n_batch // 2
    sem = pltpu.SemaphoreType.DMA
    f32, bf16 = jnp.float32, jnp.bfloat16
    any_spec = pl.BlockSpec(memory_space=pl.ANY)
    return pl.pallas_call(
        functools.partial(fused_kernel, n_batch),
        out_shape=(jax.ShapeDtypeStruct(query.shape, bf16), jax.ShapeDtypeStruct(query.shape, bf16),
                   jax.ShapeDtypeStruct((2, n_batch, 2, PIECE, DIM), bf16),
                   jax.ShapeDtypeStruct((2, n_batch, 2, PIECE, DIM), bf16)),
        in_specs=[any_spec] * 5,
        out_specs=(any_spec,) * 4,
        scratch_shapes=[
            pltpu.VMEM((Q_RING, 4, 2, PIECE, GROUP, DIM), bf16),
            pltpu.VMEM((Q_RING, 4, 2, PIECE, GROUP, DIM), bf16),
            pltpu.VMEM((4, CS_RING, 2, PIECE, DIM), f32),
            pltpu.VMEM((2 * CP, n_batch, 2, PIECE, DIM), bf16),
            pltpu.VMEM((S1_RING, 4, 2, DIM, DIM), f32),
            pltpu.VMEM((S2_RING, 2, 2, DIM, DIM), f32),
            pltpu.VMEM((PARTS, 2, 8, DIM, DIM), f32),
            pltpu.VMEM((2, 2, 4, PIECE, GROUP, DIM), bf16),
            pltpu.VMEM((2, 2, 4, PIECE, DIM), bf16),
            pltpu.VMEM((2 * CP * PIECE, DIM), bf16),
            pltpu.VMEM((2 * CP * PIECE, DIM), bf16),
            sem((n_groups, 2)), sem((n_groups, CP, 2)), sem((n_groups, CP, 2)), sem((n_groups, 2, 2, 2)),
            sem((n_groups, 4, 2)), sem((n_groups, 4, 2)), sem((n_groups, 4, 2)),
            sem((PARTS, 4)), sem((n_batch, 4)), sem((n_batch, 2)), sem((n_batch, 2)),
            sem((2, 2, 2)), sem((2, 2, 2)), sem((n_batch, 2, 2)),
            sem((2, 2, 2)), sem((2, 2, 2)), sem((n_batch, 2, 2)),
        ],
        compiler_params=pltpu.CompilerParams(collective_id=0, has_side_effects=True, vmem_limit_bytes=VMEM_MIB * 2 ** 20),
    )(query, grad_out, cos_t, sin_t, kv)


def hand_on_kernel(a_ref, b_ref, sem):
    copy = pltpu.make_async_copy(a_ref, b_ref, sem)
    copy.start()
    copy.wait()


def hand_on(a):
    any_spec = pl.BlockSpec(memory_space=pl.ANY)
    return pl.pallas_call(hand_on_kernel, in_specs=[any_spec], out_specs=any_spec,
                          out_shape=jax.ShapeDtypeStruct(a.shape, a.dtype),
                          scratch_shapes=[pltpu.SemaphoreType.DMA(())],
                          compiler_params=pltpu.CompilerParams(vmem_limit_bytes=2 ** 20))(a)


def cos_sin(angles):
    turns = jnp.floor(angles * (2.0 / math.pi) + 0.5)
    rest = ((angles - turns * 1.5703125) - turns * 4.837512969970703125e-4) - turns * 7.549789948768648e-8
    sq = rest * rest
    sine = ((-1.9515295891e-4 * sq + 8.3321608736e-3) * sq - 1.6666654611e-1) * sq * rest + rest
    cosine = ((2.443315711809948e-5 * sq - 1.388731625493765e-3) * sq + 4.166664568298827e-2) * sq * sq - 0.5 * sq + 1.0
    quarter = turns.astype(jnp.int32) % 4
    odd = quarter % 2 == 1
    cos_v = jnp.where(odd, sine, cosine)
    sin_v = jnp.where(odd, cosine, sine)
    cos_v = jnp.where((quarter == 1) | (quarter == 2), -cos_v, cos_v)
    sin_v = jnp.where(quarter >= 2, -sin_v, sin_v)
    return cos_v, sin_v


def solution(mesh):
    head_spec = P(None, 'cp', 'tp', None)
    pos_spec = P(None, 'cp')

    def local_step(query, keys, values, positions, grad_out):
        batch, length, n_heads, dim = query.shape
        lanes = jnp.arange(dim, dtype=jnp.int32)
        freq_expo = (lanes // 2).astype(jnp.float32) * (2.0 / dim)
        inv_freq = 1.0 / (ROPE_THETA ** freq_expo)
        angles = positions.astype(jnp.float32)[:, :, None] * inv_freq
        cos_t, sin_t = cos_sin(angles)
        sin_t = sin_t * jnp.where(lanes % 2 == 0, -1.0, 1.0)
        cos_t, sin_t = lax.optimization_barrier((cos_t, sin_t))
        swap_mat = (lanes[:, None] == (lanes ^ 1)[None, :]).astype(jnp.bfloat16)
        k_t = keys.transpose(2, 0, 1, 3)
        k_swap = jnp.einsum('hbtd,de->hbte', k_t, swap_mat, preferred_element_type=jnp.float32)
        k_rot = (k_t.astype(jnp.float32) * cos_t + k_swap * sin_t).astype(jnp.bfloat16)
        by_half = (2, batch, 2, PIECE, dim)
        kv = jnp.stack([k_rot.reshape(by_half), values.transpose(2, 0, 1, 3).reshape(by_half)], axis=3)
        kv = kv.transpose(0, 2, 1, 3, 4, 5)
        split = (batch, 2, PIECE, 2, GROUP, dim)
        out, dq, dk, dv = fused_attention(query.reshape(split), grad_out.reshape(split), cos_t.reshape(by_half[1:]),
                                          sin_t.reshape(by_half[1:]), kv)
        out, dq = hand_on(out), hand_on(dq)
        back = (2, batch, length, dim)
        return out.reshape(query.shape), dq.reshape(query.shape), dk.reshape(back).transpose(1, 2, 0, 3), dv.reshape(back).transpose(1, 2, 0, 3)

    return jax.shard_map(local_step, mesh=mesh,
                         in_specs=(head_spec, head_spec, head_spec, pos_spec, head_spec),
                         out_specs=(head_spec, head_spec, head_spec, head_spec), check_vma=False)
```

```python
import functools
import math

import jax
import jax.numpy as jnp
from jax import lax
from jax.experimental import pallas as pl
from jax.experimental.pallas import tpu as pltpu
from jax.sharding import PartitionSpec as P

ROPE_THETA = 1000000.0
LOG2E = 1.4426950408889634
MESH = pl.DeviceIdType.MESH
CP = 8
PIECE = 64
GROUP = 8
DIM = 128
PARTS = 4
LAG_ADD = 3
LAG_END = 5
KEY_BLOCK = 256
VMEM_MIB = 36
Q_RING = 3
CS_RING = 12
S1_RING = 10
S2_RING = 6


def swap_pairs(x):
    lane = lax.broadcasted_iota(jnp.int32, x.shape, 1)
    return jnp.where(lane % 2 == 0, pltpu.roll(x, 127, 1), pltpu.roll(x, 1, 1))


def dot_nt(a, b):
    return lax.dot_general(a, b, (((1,), (1,)), ((), ())), preferred_element_type=jnp.float32)


def dot_nn(a, b):
    return lax.dot_general(a, b, (((1,), (0,)), ((), ())), preferred_element_type=jnp.float32)


def attend_tile(qr, gr, k_view, v_view, n_keys, q_start, scale):
    n_blk = n_keys // KEY_BLOCK
    scores = []
    for j in range(n_blk):
        s = dot_nt(qr, k_view[j * KEY_BLOCK:(j + 1) * KEY_BLOCK, :])
        if j == n_blk - 1:
            q_idx = q_start + lax.broadcasted_iota(jnp.int32, s.shape, 0) // GROUP
            k_idx = j * KEY_BLOCK + lax.broadcasted_iota(jnp.int32, s.shape, 1)
            s = jnp.where(k_idx <= q_idx, s, -jnp.inf)
        scores.append(s)
    row_max = jnp.max(functools.reduce(jnp.maximum, scores), axis=1, keepdims=True)
    expo = [jnp.exp2((s - row_max) * (scale * LOG2E)) for s in scores]
    row_sum = jnp.sum(functools.reduce(jnp.add, expo), axis=1, keepdims=True)
    inv = 1.0 / row_sum
    probs = [e * inv for e in expo]
    p_all = jnp.concatenate([p.astype(jnp.bfloat16) for p in probs], axis=1)
    out = dot_nn(p_all, v_view[0:n_keys, :])
    delta = jnp.sum(out * gr.astype(jnp.float32), axis=1, keepdims=True)
    ds = []
    for j in range(n_blk):
        dp = dot_nt(gr, v_view[j * KEY_BLOCK:(j + 1) * KEY_BLOCK, :])
        ds.append((probs[j] * (dp - delta)).astype(jnp.bfloat16))
    ds_all = jnp.concatenate(ds, axis=1)
    dq = dot_nn(ds_all, k_view[0:n_keys, :]) * scale
    dv_t = dot_nn(gr.T, p_all)
    dk_t = dot_nn(qr.T, ds_all) * scale
    return out, dq, dk_t, dv_t


def fused_kernel(n_batch, q_hbm, g_hbm, cos_hbm, sin_hbm, kv_hbm, out_hbm, dq_hbm, dk_hbm, dv_hbm,
                 q_l, g_l, cs_l, kv_l, s1_l, s2_l, part, o_st, f_st, k_s, v_s,
                 kv_loc, kv_send, kv_recv, pass_send, q_loc, q_send, q_recv, s1_send, s1_recv, s2_send, s2_recv,
                 o_loc, o_send, o_recv, f_loc, f_send, f_recv):
    me = lax.axis_index('cp')
    chip, core = me // 2, me % 2
    sibling = chip * 2 + 1 - core
    n_groups = n_batch // 2
    scale = DIM ** -0.5
    diag = 3 - chip

    def own_slot(half):
        return core if half == 0 else 3 - core

    def sib_slot(half):
        return 1 - core if half == 0 else 2 + core

    def partners(b):
        along_x = chip + 1 - 2 * (chip % 2)
        along_y = (chip + 2) % 4
        odd = b % 2
        return along_x * (1 - odd) + along_y * odd, along_y * (1 - odd) + along_x * odd

    def remote(src, dst, send, recv, device):
        return pltpu.make_async_remote_copy(src_ref=src, dst_ref=dst, send_sem=send, recv_sem=recv,
                                            device_id={'cp': device}, device_id_type=MESH)

    def kv_piece(device, half):
        return device if half == 0 else 2 * CP - 1 - device

    def kv_copy(g, dest, half):
        pair = pl.ds(g * 2, 2)
        return remote(kv_hbm.at[dest % 2, half, pair], kv_l.at[kv_piece(me, half), pair],
                      kv_send.at[g, dest, half], kv_recv.at[g, me, half], dest)

    def kv_own(g, half):
        pair = pl.ds(g * 2, 2)
        return pltpu.make_async_copy(kv_hbm.at[core, half, pair], kv_l.at[kv_piece(me, half), pair], kv_loc.at[g, half])

    near_x = chip + 1 - 2 * (chip % 2)
    near_y = (chip + 2) % 4
    near = (sibling, near_x * 2, near_x * 2 + 1, near_y * 2, near_y * 2 + 1)
    far = (diag * 2, diag * 2 + 1)

    def kv_arrive(g, source, half):
        pair = pl.ds(g * 2, 2)
        return remote(kv_hbm.at[core, half, pair], kv_l.at[kv_piece(source, half), pair],
                      kv_send.at[g, source, half], kv_recv.at[g, source, half], source)

    def kv_each(g, do):
        for dest in near:
            do(kv_copy(g, dest, 0))

            @pl.when(dest // 2 <= chip)
            def _(dest=dest):
                do(kv_copy(g, dest, 1))

        @pl.when(chip == 2)
        def _():
            for dest in far:
                do(kv_copy(g, dest, 1))

    def kv_issue(g):
        for half in range(2):
            kv_own(g, half).start()
        kv_each(g, lambda copy: copy.start())

    def kv_wait_from(g, sources):
        for source in sources:
            kv_arrive(g, source, 0).wait_recv()

            @pl.when(chip <= source // 2)
            def _(source=source):
                kv_arrive(g, source, 1).wait_recv()

    def kv_pass(g, i, source_chip, source_core, half):
        pair = pl.ds(g * 2, 2)
        source = source_chip * 2 + source_core
        place = kv_l.at[kv_piece(source, half), pair]
        return remote(place, place, pass_send.at[g, i, source_core, half], kv_recv.at[g, source, half],
                      (3 - source_chip) * 2 + core)

    def kv_pass_each(g, do):
        from_last = (g + chip + 1) % 2

        @pl.when(jnp.logical_or(chip == 1, chip == 2))
        def _():
            for source_core in range(2):
                do(kv_pass(g, 0, 3 * from_last, source_core, 0))

                @pl.when(from_last == 1)
                def _(source_core=source_core):
                    do(kv_pass(g, 0, 3 * from_last, source_core, 1))

        @pl.when(chip == 3)
        def _():
            for i in range(2):
                for source_core in range(2):
                    do(kv_pass(g, i, 1 + i, source_core, 0))

    def kv_near(g):
        kv_wait_from(g, near)
        kv_pass_each(g, lambda copy: copy.start())

    def kv_far(g):
        for half in range(2):
            kv_own(g, half).wait()
        kv_wait_from(g, far)

    def kv_drain(g):
        kv_each(g, lambda copy: copy.wait_send())
        kv_pass_each(g, lambda copy: copy.wait_send())

    def q_views(g, half, slot, head):
        pair = pl.ds(g * 2, 2)
        ring = g % Q_RING
        held = pl.ds(g % (CS_RING // 2) * 2, 2)
        return ((q_hbm.at[pair, half, :, head], q_l.at[ring, slot]),
                (g_hbm.at[pair, half, :, head], g_l.at[ring, slot]),
                (cos_hbm.at[pair, half], cs_l.at[slot, held, 0]),
                (sin_hbm.at[pair, half], cs_l.at[slot, held, 1]))

    def q_local(g):
        return [pltpu.make_async_copy(src, dst, q_loc.at[g, i, half]) for half in range(2)
                for i, (src, dst) in enumerate(q_views(g, half, own_slot(half), core))]

    def q_out(g):
        return [remote(src, dst, q_send.at[g, i, half], q_recv.at[g, i, half], sibling) for half in range(2)
                for i, (src, dst) in enumerate(q_views(g, half, own_slot(half), 1 - core))]

    def q_arriving(g):
        return [remote(src, dst, q_send.at[g, i, half], q_recv.at[g, i, half], sibling) for half in range(2)
                for i, (src, dst) in enumerate(q_views(g, half, sib_slot(half), core))]

    def q_issue(g):
        for copy in q_local(g) + q_out(g):
            copy.start()

    def q_wait(g):
        for copy in q_local(g):
            copy.wait()
        for copy in q_arriving(g):
            copy.wait_recv()

    def o_local(b):
        return [pltpu.make_async_copy(o_st.at[b % 2, a, own_slot(half)], ref.at[b, half, :, core],
                                      o_loc.at[b % 2, a, half])
                for a, ref in enumerate((out_hbm, dq_hbm)) for half in range(2)]

    def o_out(b):
        return [remote(o_st.at[b % 2, a, sib_slot(half)], ref.at[b, half, :, core],
                       o_send.at[b % 2, a, half], o_recv.at[b, a, half], sibling)
                for a, ref in enumerate((out_hbm, dq_hbm)) for half in range(2)]

    def o_drain(b):
        for copy in o_local(b):
            copy.wait()
        for copy in o_out(b):
            copy.wait_send()

    def o_wait(b):
        for a, ref in enumerate((out_hbm, dq_hbm)):
            for half in range(2):
                remote(o_st.at[b % 2, a, own_slot(half)], ref.at[b, half, :, 1 - core],
                       o_send.at[b % 2, a, half], o_recv.at[b, a, half], sibling).wait_recv()

    def f_local(b):
        return [pltpu.make_async_copy(f_st.at[b % 2, a, own_slot(half)], ref.at[core, b, half], f_loc.at[b % 2, a, half])
                for a, ref in enumerate((dk_hbm, dv_hbm)) for half in range(2)]

    def f_out(b):
        return [remote(f_st.at[b % 2, a, sib_slot(half)], ref.at[core, b, half],
                       f_send.at[b % 2, a, half], f_recv.at[b, a, half], sibling)
                for a, ref in enumerate((dk_hbm, dv_hbm)) for half in range(2)]

    def f_drain(b):
        for copy in f_local(b):
            copy.wait()
        for copy in f_out(b):
            copy.wait_send()

    def f_wait(b):
        for a, ref in enumerate((dk_hbm, dv_hbm)):
            for half in range(2):
                remote(f_st.at[b % 2, a, own_slot(half)], ref.at[1 - core, b, half],
                       f_send.at[b % 2, a, half], f_recv.at[b, a, half], sibling).wait_recv()

    def s1_copy(b, m):
        first, _ = partners(b)
        target = first if m < 2 else diag
        block = target if m % 2 == 0 else 7 - target
        return remote(part.at[b % PARTS, :, block], s1_l.at[b % S1_RING, m], s1_send.at[b % PARTS, m], s1_recv.at[b, m],
                      first * 2 + core)

    def s1_high(b, do):
        first, _ = partners(b)
        for m, target in ((1, first), (3, diag)):
            @pl.when(target > chip)
            def _(m=m):
                do(s1_copy(b, m))

    def s1_low(b, do):
        for m in (0, 2):
            do(s1_copy(b, m))

    def s1_each(b, do):
        s1_high(b, do)
        s1_low(b, do)

    def s2_copy(b, m):
        _, second = partners(b)
        return remote(s1_l.at[b % S1_RING, 2 + m], s2_l.at[b % S2_RING, m], s2_send.at[b, m], s2_recv.at[b, m], second * 2 + core)

    def s2_send_high(b):
        first, second = partners(b)
        return jnp.logical_or(second > chip, second > first)

    def s2_recv_high(b):
        _, second = partners(b)
        return jnp.logical_or(chip > second, chip > diag)

    def s2_each(b, do):
        do(s2_copy(b, 0))

        @pl.when(s2_send_high(b))
        def _():
            do(s2_copy(b, 1))

    def add_step(b):
        first, second = partners(b)
        ring = b % PARTS
        s1_copy(b, 0).wait_recv()
        s1_copy(b, 2).wait_recv()

        @pl.when(chip > first)
        def _():
            s1_copy(b, 1).wait_recv()

        @pl.when(second > first)
        def _():
            s1_copy(b, 3).wait_recv()

        at = b % S1_RING
        for i in range(2):
            s1_l[at, 0, i] = s1_l[at, 0, i] + part[ring, i, chip]
            s1_l[at, 2, i] = s1_l[at, 2, i] + part[ring, i, second]
            s1_l[at, 1, i] = jnp.where(chip > first, s1_l[at, 1, i], 0.0) + part[ring, i, 7 - chip]
            s1_l[at, 3, i] = jnp.where(second > first, s1_l[at, 3, i], 0.0) + part[ring, i, 7 - second]

    def end_step(b):
        s2_copy(b, 0).wait_recv()
        has_high = s2_recv_high(b)

        @pl.when(has_high)
        def _():
            s2_copy(b, 1).wait_recv()

        @pl.when(b >= 2)
        def _():
            f_drain(b - 2)

        s2_each(b, lambda copy: copy.wait_send())
        ring = b % 2
        for m in range(2):
            for i in range(2):
                other = s2_l[b % S2_RING, m, i]
                if m == 1:
                    other = jnp.where(has_high, other, 0.0)
                total = (s1_l[b % S1_RING, m, i] + other).T
                for sub in range(2):
                    slot = m * 2 + sub
                    x = total[sub * PIECE:(sub + 1) * PIECE]
                    if i == 0:
                        x = x * cs_l[slot, b % CS_RING, 0] - swap_pairs(x) * cs_l[slot, b % CS_RING, 1]
                    f_st[ring, i, slot] = x.astype(jnp.bfloat16)

    def compute(b):
        ring, g_ring, b_in, c_ring = b % PARTS, (b // 2) % Q_RING, b % 2, b % CS_RING

        @pl.when(b >= PARTS)
        def _():
            s1_each(b - PARTS, lambda copy: copy.wait_send())

        @pl.when(b >= 2)
        def _():
            o_drain(b - 2)

        for piece in range(2 * CP):
            k_p, v_p = kv_l[piece, b, 0], kv_l[piece, b, 1]
            if piece >= CP:
                needed = (2 * CP - 1 - piece) // 2 >= chip
                k_p, v_p = jnp.where(needed, k_p, 0), jnp.where(needed, v_p, 0)
            k_s[piece * PIECE:(piece + 1) * PIECE, :] = k_p.astype(jnp.bfloat16)
            v_s[piece * PIECE:(piece + 1) * PIECE, :] = v_p.astype(jnp.bfloat16)
        for i in range(2):
            for j in range(8):
                part[ring, i, j] = jnp.zeros((DIM, DIM), jnp.float32)

        def tile(slot, n_keys, q_start):
            rows = PIECE * GROUP
            cos = jnp.broadcast_to(cs_l[slot, c_ring, 0][:, None, :], (PIECE, GROUP, DIM)).reshape(rows, DIM)
            sin = jnp.broadcast_to(cs_l[slot, c_ring, 1][:, None, :], (PIECE, GROUP, DIM)).reshape(rows, DIM)
            qx = q_l[g_ring, slot, b_in].astype(jnp.float32).reshape(rows, DIM)
            qr = (qx * cos + swap_pairs(qx) * sin).astype(jnp.bfloat16)
            gr = g_l[g_ring, slot, b_in].astype(jnp.float32).reshape(rows, DIM).astype(jnp.bfloat16)
            out, dq, dk_t, dv_t = attend_tile(qr, gr, k_s, v_s, n_keys, q_start, scale)
            dq = dq * cos - swap_pairs(dq) * sin
            o_st[b % 2, 0, slot] = out.reshape(PIECE, GROUP, DIM).astype(jnp.bfloat16)
            o_st[b % 2, 1, slot] = dq.reshape(PIECE, GROUP, DIM).astype(jnp.bfloat16)
            for j in reversed(range(n_keys // DIM)):
                part[ring, 0, j] += dk_t[:, j * DIM:(j + 1) * DIM]
                part[ring, 1, j] += dv_t[:, j * DIM:(j + 1) * DIM]

        def high(n_keys):
            def body(i, carry):
                tile(2 + i, n_keys, (2 * CP - 2 - 2 * chip + i) * PIECE)
                return carry

            lax.fori_loop(0, 2, body, 0)

        def low(n_keys):
            def body(i, carry):
                tile(i, n_keys, (2 * chip + i) * PIECE)
                return carry

            lax.fori_loop(0, 2, body, 0)

        @pl.when(chip < 2)
        def _():
            high(2 * CP * PIECE)

        @pl.when(chip >= 2)
        def _():
            high(CP * PIECE * 3 // 2)

        s1_high(b, lambda copy: copy.start())

        @pl.when(chip < 2)
        def _():
            low(CP * PIECE // 2)

        @pl.when(chip >= 2)
        def _():
            low(CP * PIECE)

    barrier = pltpu.get_barrier_semaphore()
    for step in range(1, CP):
        pl.semaphore_signal(barrier, inc=1, device_id={'cp': (me + step) % CP}, device_id_type=MESH)
    pl.semaphore_wait(barrier, CP - 1)

    kv_issue(0)
    q_issue(0)
    kv_near(0)
    kv_issue(1)

    def step(it, carry):
        even = it % 2 == 0

        @pl.when(jnp.logical_and(even, jnp.logical_and(it >= 4, it + 2 < n_batch)))
        def _():
            o_wait(it - 4)
            o_wait(it - 3)

        @pl.when(jnp.logical_and(even, it + 2 < n_batch))
        def _():
            q_issue(it // 2 + 1)

        @pl.when(jnp.logical_and(even, it // 2 + 2 < n_groups))
        def _():
            kv_issue(it // 2 + 2)

        @pl.when(jnp.logical_and(it >= LAG_ADD, it < n_batch + LAG_ADD))
        def _():
            add_step(it - LAG_ADD)

        @pl.when(it >= LAG_END)
        def _():
            end_step(it - LAG_END)

        @pl.when(jnp.logical_and(it >= LAG_ADD, it < n_batch + LAG_ADD))
        def _():
            s2_each(it - LAG_ADD, lambda copy: copy.start())

        @pl.when(jnp.logical_and(even, it < n_batch))
        def _():
            kv_far(it // 2)
            q_wait(it // 2)

        @pl.when(it < n_batch)
        def _():
            compute(it)

            @pl.when(jnp.logical_and(even, it // 2 + 1 < n_groups))
            def _():
                kv_near(it // 2 + 1)

            s1_low(it, lambda copy: copy.start())
            for copy in o_local(it) + o_out(it):
                copy.start()

        @pl.when(it >= LAG_END)
        def _():
            for copy in f_local(it - LAG_END) + f_out(it - LAG_END):
                copy.start()

        return carry

    lax.fori_loop(0, n_batch + LAG_END, step, 0)

    for b in range(n_batch - PARTS, n_batch):
        s1_each(b, lambda copy: copy.wait_send())
    for b in range(n_batch - 2, n_batch):
        o_drain(b)
        f_drain(b)

    def drain_group(g, carry):
        kv_drain(g)
        for copy in q_out(g):
            copy.wait_send()
        return carry

    def drain_batch(b, carry):
        f_wait(b)
        return carry

    def drain_out(b, carry):
        o_wait(b)
        return carry

    lax.fori_loop(0, n_groups, drain_group, 0)
    lax.fori_loop(0, n_batch, drain_batch, 0)
    lax.fori_loop(n_batch - 6, n_batch, drain_out, 0)


def fused_attention(query, grad_out, cos_t, sin_t, kv):
    n_batch = query.shape[0]
    n_groups = n_batch // 2
    sem = pltpu.SemaphoreType.DMA
    f32, bf16 = jnp.float32, jnp.bfloat16
    any_spec = pl.BlockSpec(memory_space=pl.ANY)
    return pl.pallas_call(
        functools.partial(fused_kernel, n_batch),
        out_shape=(jax.ShapeDtypeStruct(query.shape, bf16), jax.ShapeDtypeStruct(query.shape, bf16),
                   jax.ShapeDtypeStruct((2, n_batch, 2, PIECE, DIM), bf16),
                   jax.ShapeDtypeStruct((2, n_batch, 2, PIECE, DIM), bf16)),
        in_specs=[any_spec] * 5,
        out_specs=(any_spec,) * 4,
        scratch_shapes=[
            pltpu.VMEM((Q_RING, 4, 2, PIECE, GROUP, DIM), bf16),
            pltpu.VMEM((Q_RING, 4, 2, PIECE, GROUP, DIM), bf16),
            pltpu.VMEM((4, CS_RING, 2, PIECE, DIM), f32),
            pltpu.VMEM((2 * CP, n_batch, 2, PIECE, DIM), bf16),
            pltpu.VMEM((S1_RING, 4, 2, DIM, DIM), f32),
            pltpu.VMEM((S2_RING, 2, 2, DIM, DIM), f32),
            pltpu.VMEM((PARTS, 2, 8, DIM, DIM), f32),
            pltpu.VMEM((2, 2, 4, PIECE, GROUP, DIM), bf16),
            pltpu.VMEM((2, 2, 4, PIECE, DIM), bf16),
            pltpu.VMEM((2 * CP * PIECE, DIM), bf16),
            pltpu.VMEM((2 * CP * PIECE, DIM), bf16),
            sem((n_groups, 2)), sem((n_groups, CP, 2)), sem((n_groups, CP, 2)), sem((n_groups, 2, 2, 2)),
            sem((n_groups, 4, 2)), sem((n_groups, 4, 2)), sem((n_groups, 4, 2)),
            sem((PARTS, 4)), sem((n_batch, 4)), sem((n_batch, 2)), sem((n_batch, 2)),
            sem((2, 2, 2)), sem((2, 2, 2)), sem((n_batch, 2, 2)),
            sem((2, 2, 2)), sem((2, 2, 2)), sem((n_batch, 2, 2)),
        ],
        compiler_params=pltpu.CompilerParams(collective_id=0, has_side_effects=True, vmem_limit_bytes=VMEM_MIB * 2 ** 20),
    )(query, grad_out, cos_t, sin_t, kv)


def hand_on_kernel(a_ref, b_ref, sem):
    copy = pltpu.make_async_copy(a_ref, b_ref, sem)
    copy.start()
    copy.wait()


def hand_on(a):
    any_spec = pl.BlockSpec(memory_space=pl.ANY)
    return pl.pallas_call(hand_on_kernel, in_specs=[any_spec], out_specs=any_spec,
                          out_shape=jax.ShapeDtypeStruct(a.shape, a.dtype),
                          scratch_shapes=[pltpu.SemaphoreType.DMA(())],
                          compiler_params=pltpu.CompilerParams(vmem_limit_bytes=2 ** 20))(a)


def cos_sin(angles):
    turns = jnp.floor(angles * (2.0 / math.pi) + 0.5)
    rest = ((angles - turns * 1.5703125) - turns * 4.837512969970703125e-4) - turns * 7.549789948768648e-8
    sq = rest * rest
    sine = ((-1.9515295891e-4 * sq + 8.3321608736e-3) * sq - 1.6666654611e-1) * sq * rest + rest
    cosine = ((2.443315711809948e-5 * sq - 1.388731625493765e-3) * sq + 4.166664568298827e-2) * sq * sq - 0.5 * sq + 1.0
    quarter = turns.astype(jnp.int32) % 4
    odd = quarter % 2 == 1
    cos_v = jnp.where(odd, sine, cosine)
    sin_v = jnp.where(odd, cosine, sine)
    cos_v = jnp.where((quarter == 1) | (quarter == 2), -cos_v, cos_v)
    sin_v = jnp.where(quarter >= 2, -sin_v, sin_v)
    return cos_v, sin_v


def solution(mesh):
    head_spec = P(None, 'cp', 'tp', None)
    pos_spec = P(None, 'cp')

    def local_step(query, keys, values, positions, grad_out):
        batch, length, n_heads, dim = query.shape
        lanes = jnp.arange(dim, dtype=jnp.int32)
        freq_expo = (lanes // 2).astype(jnp.float32) * (2.0 / dim)
        inv_freq = 1.0 / (ROPE_THETA ** freq_expo)
        angles = positions.astype(jnp.float32)[:, :, None] * inv_freq
        cos_t, sin_t = cos_sin(angles)
        sin_t = sin_t * jnp.where(lanes % 2 == 0, -1.0, 1.0)
        cos_t, sin_t = lax.optimization_barrier((cos_t, sin_t))
        swap_mat = (lanes[:, None] == (lanes ^ 1)[None, :]).astype(jnp.bfloat16)
        k_t = keys.transpose(2, 0, 1, 3)
        k_swap = jnp.einsum('hbtd,de->hbte', k_t, swap_mat, preferred_element_type=jnp.float32)
        k_rot = (k_t.astype(jnp.float32) * cos_t + k_swap * sin_t).astype(jnp.bfloat16)
        by_half = (2, batch, 2, PIECE, dim)
        kv = jnp.stack([k_rot.reshape(by_half), values.transpose(2, 0, 1, 3).reshape(by_half)], axis=3)
        kv = kv.transpose(0, 2, 1, 3, 4, 5)
        split = (batch, 2, PIECE, 2, GROUP, dim)
        out, dq, dk, dv = fused_attention(query.reshape(split), grad_out.reshape(split), cos_t.reshape(by_half[1:]),
                                          sin_t.reshape(by_half[1:]), kv)
        out, dq = hand_on(out), hand_on(dq)
        back = (2, batch, length, dim)
        return out.reshape(query.shape), dq.reshape(query.shape), dk.reshape(back).transpose(1, 2, 0, 3), dv.reshape(back).transpose(1, 2, 0, 3)

    return jax.shard_map(local_step, mesh=mesh,
                         in_specs=(head_spec, head_spec, head_spec, pos_spec, head_spec),
                         out_specs=(head_spec, head_spec, head_spec, head_spec), check_vma=False)
```

```python
import functools
import math

import jax
import jax.numpy as jnp
from jax import lax
from jax.experimental import pallas as pl
from jax.experimental.pallas import tpu as pltpu
from jax.sharding import PartitionSpec as P

ROPE_THETA = 1000000.0
LOG2E = 1.4426950408889634
MESH = pl.DeviceIdType.MESH
CP = 8
PIECE = 64
GROUP = 8
DIM = 128
PARTS = 4
LAG_ADD = 3
LAG_END = 5
KEY_BLOCK = 256
VMEM_MIB = 36
Q_RING = 3
CS_RING = 12
S1_RING = 10
S2_RING = 6


def swap_pairs(x):
    lane = lax.broadcasted_iota(jnp.int32, x.shape, 1)
    return jnp.where(lane % 2 == 0, pltpu.roll(x, 127, 1), pltpu.roll(x, 1, 1))


def dot_nt(a, b):
    return lax.dot_general(a, b, (((1,), (1,)), ((), ())), preferred_element_type=jnp.float32)


def dot_nn(a, b):
    return lax.dot_general(a, b, (((1,), (0,)), ((), ())), preferred_element_type=jnp.float32)


def attend_tile(qr, gr, k_view, v_view, n_keys, q_start, scale):
    n_blk = n_keys // KEY_BLOCK
    scores = []
    for j in range(n_blk):
        s = dot_nt(qr, k_view[j * KEY_BLOCK:(j + 1) * KEY_BLOCK, :])
        if j == n_blk - 1:
            q_idx = q_start + lax.broadcasted_iota(jnp.int32, s.shape, 0) // GROUP
            k_idx = j * KEY_BLOCK + lax.broadcasted_iota(jnp.int32, s.shape, 1)
            s = jnp.where(k_idx <= q_idx, s, -jnp.inf)
        scores.append(s)
    row_max = jnp.max(functools.reduce(jnp.maximum, scores), axis=1, keepdims=True)
    expo = [jnp.exp2((s - row_max) * (scale * LOG2E)) for s in scores]
    row_sum = jnp.sum(functools.reduce(jnp.add, expo), axis=1, keepdims=True)
    inv = 1.0 / row_sum
    probs = [e * inv for e in expo]
    p_all = jnp.concatenate([p.astype(jnp.bfloat16) for p in probs], axis=1)
    out = dot_nn(p_all, v_view[0:n_keys, :])
    delta = jnp.sum(out * gr.astype(jnp.float32), axis=1, keepdims=True)
    ds = []
    for j in range(n_blk):
        dp = dot_nt(gr, v_view[j * KEY_BLOCK:(j + 1) * KEY_BLOCK, :])
        ds.append((probs[j] * (dp - delta)).astype(jnp.bfloat16))
    ds_all = jnp.concatenate(ds, axis=1)
    dq = dot_nn(ds_all, k_view[0:n_keys, :]) * scale
    dv_t = dot_nn(gr.T, p_all)
    dk_t = dot_nn(qr.T, ds_all) * scale
    return out, dq, dk_t, dv_t


def fused_kernel(n_batch, q_hbm, g_hbm, cos_hbm, sin_hbm, kv_hbm, out_hbm, dq_hbm, dk_hbm, dv_hbm,
                 q_l, g_l, cs_l, kv_l, s1_l, s2_l, part, o_st, f_st, k_s, v_s,
                 kv_loc, kv_send, kv_recv, q_loc, q_send, q_recv, s1_send, s1_recv, s2_send, s2_recv,
                 o_loc, o_send, o_recv, f_loc, f_send, f_recv):
    me = lax.axis_index('cp')
    chip, core = me // 2, me % 2
    sibling = chip * 2 + 1 - core
    n_groups = n_batch // 2
    scale = DIM ** -0.5
    diag = 3 - chip

    def own_slot(half):
        return core if half == 0 else 3 - core

    def sib_slot(half):
        return 1 - core if half == 0 else 2 + core

    def partners(b):
        along_x = chip + 1 - 2 * (chip % 2)
        along_y = (chip + 2) % 4
        odd = b % 2
        return along_x * (1 - odd) + along_y * odd, along_y * (1 - odd) + along_x * odd

    def remote(src, dst, send, recv, device):
        return pltpu.make_async_remote_copy(src_ref=src, dst_ref=dst, send_sem=send, recv_sem=recv,
                                            device_id={'cp': device}, device_id_type=MESH)

    def kv_piece(device, half):
        return device if half == 0 else 2 * CP - 1 - device

    def kv_copy(g, dest, half):
        pair = pl.ds(g * 2, 2)
        return remote(kv_hbm.at[dest % 2, half, pair], kv_l.at[kv_piece(me, half), pair],
                      kv_send.at[g, dest, half], kv_recv.at[g, me, half], dest)

    def kv_own(g, half):
        pair = pl.ds(g * 2, 2)
        return pltpu.make_async_copy(kv_hbm.at[core, half, pair], kv_l.at[kv_piece(me, half), pair], kv_loc.at[g, half])

    def kv_arrive(g, source, half):
        pair = pl.ds(g * 2, 2)
        return remote(kv_hbm.at[core, half, pair], kv_l.at[kv_piece(source, half), pair],
                      kv_send.at[g, source, half], kv_recv.at[g, source, half], source)

    def kv_issue(g):
        for half in range(2):
            kv_own(g, half).start()
        for step in range(1, CP):
            dest = (me + step) % CP
            kv_copy(g, dest, 0).start()

            @pl.when(dest // 2 <= chip)
            def _():
                kv_copy(g, dest, 1).start()

    def kv_wait(g):
        for half in range(2):
            kv_own(g, half).wait()
        for step in range(1, CP):
            source = (me + step) % CP
            kv_arrive(g, source, 0).wait_recv()

            @pl.when(chip <= source // 2)
            def _():
                kv_arrive(g, source, 1).wait_recv()

    def kv_drain(g):
        for step in range(1, CP):
            dest = (me + step) % CP
            kv_copy(g, dest, 0).wait_send()

            @pl.when(dest // 2 <= chip)
            def _():
                kv_copy(g, dest, 1).wait_send()

    def q_views(g, half, slot, head):
        pair = pl.ds(g * 2, 2)
        ring = g % Q_RING
        held = pl.ds(g % (CS_RING // 2) * 2, 2)
        return ((q_hbm.at[pair, half, :, head], q_l.at[ring, slot]),
                (g_hbm.at[pair, half, :, head], g_l.at[ring, slot]),
                (cos_hbm.at[pair, half], cs_l.at[slot, held, 0]),
                (sin_hbm.at[pair, half], cs_l.at[slot, held, 1]))

    def q_local(g):
        return [pltpu.make_async_copy(src, dst, q_loc.at[g, i, half]) for half in range(2)
                for i, (src, dst) in enumerate(q_views(g, half, own_slot(half), core))]

    def q_out(g):
        return [remote(src, dst, q_send.at[g, i, half], q_recv.at[g, i, half], sibling) for half in range(2)
                for i, (src, dst) in enumerate(q_views(g, half, own_slot(half), 1 - core))]

    def q_arriving(g):
        return [remote(src, dst, q_send.at[g, i, half], q_recv.at[g, i, half], sibling) for half in range(2)
                for i, (src, dst) in enumerate(q_views(g, half, sib_slot(half), core))]

    def q_issue(g):
        for copy in q_local(g) + q_out(g):
            copy.start()

    def q_wait(g):
        for copy in q_local(g):
            copy.wait()
        for copy in q_arriving(g):
            copy.wait_recv()

    def o_local(b):
        return [pltpu.make_async_copy(o_st.at[b % 2, a, own_slot(half)], ref.at[b, half, :, core],
                                      o_loc.at[b % 2, a, half])
                for a, ref in enumerate((out_hbm, dq_hbm)) for half in range(2)]

    def o_out(b):
        return [remote(o_st.at[b % 2, a, sib_slot(half)], ref.at[b, half, :, core],
                       o_send.at[b % 2, a, half], o_recv.at[b, a, half], sibling)
                for a, ref in enumerate((out_hbm, dq_hbm)) for half in range(2)]

    def o_drain(b):
        for copy in o_local(b):
            copy.wait()
        for copy in o_out(b):
            copy.wait_send()

    def o_wait(b):
        for a, ref in enumerate((out_hbm, dq_hbm)):
            for half in range(2):
                remote(o_st.at[b % 2, a, own_slot(half)], ref.at[b, half, :, 1 - core],
                       o_send.at[b % 2, a, half], o_recv.at[b, a, half], sibling).wait_recv()

    def f_local(b):
        return [pltpu.make_async_copy(f_st.at[b % 2, a, own_slot(half)], ref.at[core, b, half], f_loc.at[b % 2, a, half])
                for a, ref in enumerate((dk_hbm, dv_hbm)) for half in range(2)]

    def f_out(b):
        return [remote(f_st.at[b % 2, a, sib_slot(half)], ref.at[core, b, half],
                       f_send.at[b % 2, a, half], f_recv.at[b, a, half], sibling)
                for a, ref in enumerate((dk_hbm, dv_hbm)) for half in range(2)]

    def f_drain(b):
        for copy in f_local(b):
            copy.wait()
        for copy in f_out(b):
            copy.wait_send()

    def f_wait(b):
        for a, ref in enumerate((dk_hbm, dv_hbm)):
            for half in range(2):
                remote(f_st.at[b % 2, a, own_slot(half)], ref.at[1 - core, b, half],
                       f_send.at[b % 2, a, half], f_recv.at[b, a, half], sibling).wait_recv()

    def s1_copy(b, m):
        first, _ = partners(b)
        target = first if m < 2 else diag
        block = target if m % 2 == 0 else 7 - target
        return remote(part.at[b % PARTS, :, block], s1_l.at[b % S1_RING, m], s1_send.at[b % PARTS, m], s1_recv.at[b, m],
                      first * 2 + core)

    def s1_high(b, do):
        first, _ = partners(b)
        for m, target in ((1, first), (3, diag)):
            @pl.when(target > chip)
            def _(m=m):
                do(s1_copy(b, m))

    def s1_low(b, do):
        for m in (0, 2):
            do(s1_copy(b, m))

    def s1_each(b, do):
        s1_high(b, do)
        s1_low(b, do)

    def s2_copy(b, m):
        _, second = partners(b)
        return remote(s1_l.at[b % S1_RING, 2 + m], s2_l.at[b % S2_RING, m], s2_send.at[b, m], s2_recv.at[b, m], second * 2 + core)

    def s2_send_high(b):
        first, second = partners(b)
        return jnp.logical_or(second > chip, second > first)

    def s2_recv_high(b):
        _, second = partners(b)
        return jnp.logical_or(chip > second, chip > diag)

    def s2_each(b, do):
        do(s2_copy(b, 0))

        @pl.when(s2_send_high(b))
        def _():
            do(s2_copy(b, 1))

    def add_step(b):
        first, second = partners(b)
        ring = b % PARTS
        s1_copy(b, 0).wait_recv()
        s1_copy(b, 2).wait_recv()

        @pl.when(chip > first)
        def _():
            s1_copy(b, 1).wait_recv()

        @pl.when(second > first)
        def _():
            s1_copy(b, 3).wait_recv()

        at = b % S1_RING
        for i in range(2):
            s1_l[at, 0, i] = s1_l[at, 0, i] + part[ring, i, chip]
            s1_l[at, 2, i] = s1_l[at, 2, i] + part[ring, i, second]
            s1_l[at, 1, i] = jnp.where(chip > first, s1_l[at, 1, i], 0.0) + part[ring, i, 7 - chip]
            s1_l[at, 3, i] = jnp.where(second > first, s1_l[at, 3, i], 0.0) + part[ring, i, 7 - second]

    def end_step(b):
        s2_copy(b, 0).wait_recv()
        has_high = s2_recv_high(b)

        @pl.when(has_high)
        def _():
            s2_copy(b, 1).wait_recv()

        @pl.when(b >= 2)
        def _():
            f_drain(b - 2)

        s2_each(b, lambda copy: copy.wait_send())
        ring = b % 2
        for m in range(2):
            for i in range(2):
                other = s2_l[b % S2_RING, m, i]
                if m == 1:
                    other = jnp.where(has_high, other, 0.0)
                total = (s1_l[b % S1_RING, m, i] + other).T
                for sub in range(2):
                    slot = m * 2 + sub
                    x = total[sub * PIECE:(sub + 1) * PIECE]
                    if i == 0:
                        x = x * cs_l[slot, b % CS_RING, 0] - swap_pairs(x) * cs_l[slot, b % CS_RING, 1]
                    f_st[ring, i, slot] = x.astype(jnp.bfloat16)

    def compute(b):
        ring, g_ring, b_in, c_ring = b % PARTS, (b // 2) % Q_RING, b % 2, b % CS_RING

        @pl.when(b >= PARTS)
        def _():
            s1_each(b - PARTS, lambda copy: copy.wait_send())

        @pl.when(b >= 2)
        def _():
            o_drain(b - 2)

        for piece in range(2 * CP):
            k_p, v_p = kv_l[piece, b, 0], kv_l[piece, b, 1]
            if piece >= CP:
                needed = (2 * CP - 1 - piece) // 2 >= chip
                k_p, v_p = jnp.where(needed, k_p, 0), jnp.where(needed, v_p, 0)
            k_s[piece * PIECE:(piece + 1) * PIECE, :] = k_p.astype(jnp.bfloat16)
            v_s[piece * PIECE:(piece + 1) * PIECE, :] = v_p.astype(jnp.bfloat16)
        for i in range(2):
            for j in range(8):
                part[ring, i, j] = jnp.zeros((DIM, DIM), jnp.float32)

        def tile(slot, n_keys, q_start):
            rows = PIECE * GROUP
            cos = jnp.broadcast_to(cs_l[slot, c_ring, 0][:, None, :], (PIECE, GROUP, DIM)).reshape(rows, DIM)
            sin = jnp.broadcast_to(cs_l[slot, c_ring, 1][:, None, :], (PIECE, GROUP, DIM)).reshape(rows, DIM)
            qx = q_l[g_ring, slot, b_in].astype(jnp.float32).reshape(rows, DIM)
            qr = (qx * cos + swap_pairs(qx) * sin).astype(jnp.bfloat16)
            gr = g_l[g_ring, slot, b_in].astype(jnp.float32).reshape(rows, DIM).astype(jnp.bfloat16)
            out, dq, dk_t, dv_t = attend_tile(qr, gr, k_s, v_s, n_keys, q_start, scale)
            dq = dq * cos - swap_pairs(dq) * sin
            o_st[b % 2, 0, slot] = out.reshape(PIECE, GROUP, DIM).astype(jnp.bfloat16)
            o_st[b % 2, 1, slot] = dq.reshape(PIECE, GROUP, DIM).astype(jnp.bfloat16)
            for j in reversed(range(n_keys // DIM)):
                part[ring, 0, j] += dk_t[:, j * DIM:(j + 1) * DIM]
                part[ring, 1, j] += dv_t[:, j * DIM:(j + 1) * DIM]

        def high(n_keys):
            def body(i, carry):
                tile(2 + i, n_keys, (2 * CP - 2 - 2 * chip + i) * PIECE)
                return carry

            lax.fori_loop(0, 2, body, 0)

        def low(n_keys):
            def body(i, carry):
                tile(i, n_keys, (2 * chip + i) * PIECE)
                return carry

            lax.fori_loop(0, 2, body, 0)

        @pl.when(chip < 2)
        def _():
            high(2 * CP * PIECE)

        @pl.when(chip >= 2)
        def _():
            high(CP * PIECE * 3 // 2)

        s1_high(b, lambda copy: copy.start())

        @pl.when(chip < 2)
        def _():
            low(CP * PIECE // 2)

        @pl.when(chip >= 2)
        def _():
            low(CP * PIECE)

    barrier = pltpu.get_barrier_semaphore()
    for step in range(1, CP):
        pl.semaphore_signal(barrier, inc=1, device_id={'cp': (me + step) % CP}, device_id_type=MESH)
    pl.semaphore_wait(barrier, CP - 1)

    kv_issue(0)
    q_issue(0)
    kv_issue(1)

    def step(it, carry):
        even = it % 2 == 0

        @pl.when(jnp.logical_and(even, jnp.logical_and(it >= 4, it + 2 < n_batch)))
        def _():
            o_wait(it - 4)
            o_wait(it - 3)

        @pl.when(jnp.logical_and(even, it + 2 < n_batch))
        def _():
            q_issue(it // 2 + 1)

        @pl.when(jnp.logical_and(even, it // 2 + 2 < n_groups))
        def _():
            kv_issue(it // 2 + 2)

        @pl.when(jnp.logical_and(it >= LAG_ADD, it < n_batch + LAG_ADD))
        def _():
            add_step(it - LAG_ADD)

        @pl.when(it >= LAG_END)
        def _():
            end_step(it - LAG_END)

        @pl.when(jnp.logical_and(it >= LAG_ADD, it < n_batch + LAG_ADD))
        def _():
            s2_each(it - LAG_ADD, lambda copy: copy.start())

        @pl.when(jnp.logical_and(even, it < n_batch))
        def _():
            kv_wait(it // 2)
            q_wait(it // 2)

        @pl.when(it < n_batch)
        def _():
            compute(it)
            s1_low(it, lambda copy: copy.start())
            for copy in o_local(it) + o_out(it):
                copy.start()

        @pl.when(it >= LAG_END)
        def _():
            for copy in f_local(it - LAG_END) + f_out(it - LAG_END):
                copy.start()

        return carry

    lax.fori_loop(0, n_batch + LAG_END, step, 0)

    for b in range(n_batch - PARTS, n_batch):
        s1_each(b, lambda copy: copy.wait_send())
    for b in range(n_batch - 2, n_batch):
        o_drain(b)
        f_drain(b)

    def drain_group(g, carry):
        kv_drain(g)
        for copy in q_out(g):
            copy.wait_send()
        return carry

    def drain_batch(b, carry):
        f_wait(b)
        return carry

    def drain_out(b, carry):
        o_wait(b)
        return carry

    lax.fori_loop(0, n_groups, drain_group, 0)
    lax.fori_loop(0, n_batch, drain_batch, 0)
    lax.fori_loop(n_batch - 6, n_batch, drain_out, 0)


def fused_attention(query, grad_out, cos_t, sin_t, kv):
    n_batch = query.shape[0]
    n_groups = n_batch // 2
    sem = pltpu.SemaphoreType.DMA
    f32, bf16 = jnp.float32, jnp.bfloat16
    any_spec = pl.BlockSpec(memory_space=pl.ANY)
    return pl.pallas_call(
        functools.partial(fused_kernel, n_batch),
        out_shape=(jax.ShapeDtypeStruct(query.shape, bf16), jax.ShapeDtypeStruct(query.shape, bf16),
                   jax.ShapeDtypeStruct((2, n_batch, 2, PIECE, DIM), bf16),
                   jax.ShapeDtypeStruct((2, n_batch, 2, PIECE, DIM), bf16)),
        in_specs=[any_spec] * 5,
        out_specs=(any_spec,) * 4,
        scratch_shapes=[
            pltpu.VMEM((Q_RING, 4, 2, PIECE, GROUP, DIM), bf16),
            pltpu.VMEM((Q_RING, 4, 2, PIECE, GROUP, DIM), bf16),
            pltpu.VMEM((4, CS_RING, 2, PIECE, DIM), f32),
            pltpu.VMEM((2 * CP, n_batch, 2, PIECE, DIM), bf16),
            pltpu.VMEM((S1_RING, 4, 2, DIM, DIM), f32),
            pltpu.VMEM((S2_RING, 2, 2, DIM, DIM), f32),
            pltpu.VMEM((PARTS, 2, 8, DIM, DIM), f32),
            pltpu.VMEM((2, 2, 4, PIECE, GROUP, DIM), bf16),
            pltpu.VMEM((2, 2, 4, PIECE, DIM), bf16),
            pltpu.VMEM((2 * CP * PIECE, DIM), bf16),
            pltpu.VMEM((2 * CP * PIECE, DIM), bf16),
            sem((n_groups, 2)), sem((n_groups, CP, 2)), sem((n_groups, CP, 2)),
            sem((n_groups, 4, 2)), sem((n_groups, 4, 2)), sem((n_groups, 4, 2)),
            sem((PARTS, 4)), sem((n_batch, 4)), sem((n_batch, 2)), sem((n_batch, 2)),
            sem((2, 2, 2)), sem((2, 2, 2)), sem((n_batch, 2, 2)),
            sem((2, 2, 2)), sem((2, 2, 2)), sem((n_batch, 2, 2)),
        ],
        compiler_params=pltpu.CompilerParams(collective_id=0, has_side_effects=True, vmem_limit_bytes=VMEM_MIB * 2 ** 20),
    )(query, grad_out, cos_t, sin_t, kv)


def hand_on_kernel(a_ref, b_ref, sem):
    copy = pltpu.make_async_copy(a_ref, b_ref, sem)
    copy.start()
    copy.wait()


def hand_on(a):
    any_spec = pl.BlockSpec(memory_space=pl.ANY)
    return pl.pallas_call(hand_on_kernel, in_specs=[any_spec], out_specs=any_spec,
                          out_shape=jax.ShapeDtypeStruct(a.shape, a.dtype),
                          scratch_shapes=[pltpu.SemaphoreType.DMA(())],
                          compiler_params=pltpu.CompilerParams(vmem_limit_bytes=2 ** 20))(a)


def cos_sin(angles):
    turns = jnp.floor(angles * (2.0 / math.pi) + 0.5)
    rest = ((angles - turns * 1.5703125) - turns * 4.837512969970703125e-4) - turns * 7.549789948768648e-8
    sq = rest * rest
    sine = ((-1.9515295891e-4 * sq + 8.3321608736e-3) * sq - 1.6666654611e-1) * sq * rest + rest
    cosine = ((2.443315711809948e-5 * sq - 1.388731625493765e-3) * sq + 4.166664568298827e-2) * sq * sq - 0.5 * sq + 1.0
    quarter = turns.astype(jnp.int32) % 4
    odd = quarter % 2 == 1
    cos_v = jnp.where(odd, sine, cosine)
    sin_v = jnp.where(odd, cosine, sine)
    cos_v = jnp.where((quarter == 1) | (quarter == 2), -cos_v, cos_v)
    sin_v = jnp.where(quarter >= 2, -sin_v, sin_v)
    return cos_v, sin_v


def solution(mesh):
    head_spec = P(None, 'cp', 'tp', None)
    pos_spec = P(None, 'cp')

    def local_step(query, keys, values, positions, grad_out):
        batch, length, n_heads, dim = query.shape
        lanes = jnp.arange(dim, dtype=jnp.int32)
        freq_expo = (lanes // 2).astype(jnp.float32) * (2.0 / dim)
        inv_freq = 1.0 / (ROPE_THETA ** freq_expo)
        angles = positions.astype(jnp.float32)[:, :, None] * inv_freq
        cos_t, sin_t = cos_sin(angles)
        sin_t = sin_t * jnp.where(lanes % 2 == 0, -1.0, 1.0)
        cos_t, sin_t = lax.optimization_barrier((cos_t, sin_t))
        swap_mat = (lanes[:, None] == (lanes ^ 1)[None, :]).astype(jnp.bfloat16)
        k_t = keys.transpose(2, 0, 1, 3)
        k_swap = jnp.einsum('hbtd,de->hbte', k_t, swap_mat, preferred_element_type=jnp.float32)
        k_rot = (k_t.astype(jnp.float32) * cos_t + k_swap * sin_t).astype(jnp.bfloat16)
        by_half = (2, batch, 2, PIECE, dim)
        kv = jnp.stack([k_rot.reshape(by_half), values.transpose(2, 0, 1, 3).reshape(by_half)], axis=3)
        kv = kv.transpose(0, 2, 1, 3, 4, 5)
        split = (batch, 2, PIECE, 2, GROUP, dim)
        out, dq, dk, dv = fused_attention(query.reshape(split), grad_out.reshape(split), cos_t.reshape(by_half[1:]),
                                          sin_t.reshape(by_half[1:]), kv)
        out, dq = hand_on(out), hand_on(dq)
        back = (2, batch, length, dim)
        return out.reshape(query.shape), dq.reshape(query.shape), dk.reshape(back).transpose(1, 2, 0, 3), dv.reshape(back).transpose(1, 2, 0, 3)

    return jax.shard_map(local_step, mesh=mesh,
                         in_specs=(head_spec, head_spec, head_spec, pos_spec, head_spec),
                         out_specs=(head_spec, head_spec, head_spec, head_spec), check_vma=False)
```
